512 devices in a mesh: ep: 64 (over x, z), tp: 8 (over y, core).
Axes of the slice: x: 4, y: 4, z: 16, core: 2. Of those that a mesh axis runs over, the one named last changes fastest.
Arguments:
- tokens: bfloat16 [1024, 4096], P('ep', 'tp'), may hold values from -6 to 6
- expert_ids: int32 [1024, 8], P('ep'), may hold values from 0 to 63, as said below
- route_weight: float32 [1024, 8], P('ep'), may hold values from 0.05 to 0.6
- gate_weight: bfloat16 [64, 1536, 4096], P('ep', 'tp'), may hold values from -0.09375 to 0.09375
- up_weight: bfloat16 [64, 1536, 4096], P('ep', 'tp'), may hold values from -0.09375 to 0.09375
- down_weight: bfloat16 [64, 1536, 4096], P('ep', 'tp'), may hold values from -0.21875 to 0.21875
Outputs:
- moe_out: bfloat16 [1024, 4096], P('ep', 'tp')
- act_absmax: float32 [2, 64], P(None, 'ep')
The draws below stay inside these ranges and needn't reach their ends.
Inputs may be any that keep to these rules, and one draw needn't show every extreme that they name: `expert_ids`: each row names 8 different experts. Exactly 2 experts are named more than 2 times among the rows of one index of ep, in every such block, and at most 8 times; one of them is named exactly 8 times in every block, the other reaches 8 in some block. Every other expert is named at most 2 times among the rows of one index of ep, and one of them exactly 2 times in every block.
All inputs are finite; a program needn't handle non-finite values.
Results may differ from the reference program's by a relative error of at most 0.015.
Values may be sent and summed in bfloat16 or wider, within the bound.
No kernel may reach another device: no remote copies, remote signals or barrier semaphores. Data moves between devices by JAX's collectives and lax.ppermute only.
A program may use at most 64 MiB of HBM per device.

```python
import jax
import jax.numpy as jnp
from jax import lax

D = 4096
FF = 1536
TOP = 8
TOK_DEV = 16
HOT = 2
EXPERTS = 64
CAP = 2
HOT_MOST = 8
TOKENS = 1024
N_EP = 64
N_TP = 8


def draw_expert_ids(key, part):
    blocks = TOKENS // TOK_DEV
    pick_count = TOK_DEV * TOP
    spread = EXPERTS - HOT - 1
    base_key = jax.random.fold_in(key, 7)
    order_key, reach_key, block_key = jax.random.split(base_key, 3)
    ranking = jax.random.permutation(order_key, EXPERTS).astype(jnp.int32)
    reach_block = jax.random.randint(reach_key, (), 0, blocks)
    others = ranking[HOT + 1:]

    def one_block(block_rng, number):
        cut_key, mix_key, rest_key, row_key = jax.random.split(block_rng, 4)
        cut_size = jax.random.randint(cut_key, (HOT,), 0, HOT_MOST - CAP).astype(jnp.int32)
        cut_size = cut_size.at[0].set(0)
        cut_size = jnp.where(number == reach_block, 0, cut_size)
        hot_count = HOT_MOST - cut_size
        remain = pick_count - jnp.sum(hot_count) - CAP
        base_count = remain // spread
        extra = remain - base_count * spread
        shuffled = jax.random.permutation(rest_key, others)
        rest_count = base_count + (jnp.arange(spread, dtype=jnp.int32) < extra).astype(jnp.int32)
        counts = jnp.zeros((EXPERTS,), jnp.int32).at[ranking[:HOT]].set(hot_count)
        counts = counts.at[ranking[HOT]].set(CAP).at[shuffled].set(rest_count)
        sequence = jax.random.permutation(mix_key, EXPERTS).astype(jnp.int32)
        ends = jnp.cumsum(counts[sequence])
        position = jnp.arange(pick_count, dtype=jnp.int32)
        which = jnp.sum((ends[None, :] <= position[:, None]).astype(jnp.int32), axis=1)
        named = sequence[which]
        layout = named.reshape(TOP, TOK_DEV).T
        row_order = jax.random.permutation(row_key, TOK_DEV)
        return layout[row_order]
    block_keys = jax.random.split(block_key, blocks)
    drawn = jax.vmap(one_block)(block_keys, jnp.arange(blocks, dtype=jnp.int32))
    return drawn.reshape(TOKENS, TOP).astype(jnp.int32)


def with_spikes(values, rng, source, target, blocks, factor):
    def block_of(dim):
        return (jnp.arange(values.shape[dim]) // (values.shape[dim] // blocks)).reshape((-1,) + (1,) * (values.ndim - 1 - dim))

    first = jax.random.permutation(rng, blocks)[block_of(target)]
    far = (block_of(target) + blocks // 2) % blocks
    return jnp.where((block_of(source) == first) | (block_of(source) == far), factor * values, values)


def level_of(key, shape, pieces, low, top_value):
    level, own = 1.0, jax.random.fold_in(key, 6)
    for axis_at, shards_of in pieces:
        draws = jnp.exp(jax.random.uniform(jax.random.fold_in(own, axis_at), (shards_of,), jnp.float32, low / len(pieces), top_value / len(pieces)))
        level = level * jnp.repeat(draws, shape[axis_at] // shards_of).reshape([-1 if axis == axis_at else 1 for axis in range(len(shape))])
    return level


def normal_values(rng, extent, scale, reach, cuts=(), held_as=jnp.bfloat16):
    array = jax.random.normal(rng, extent, jnp.float32) * scale
    if len(cuts) > 0:
        array = level_of(rng, extent, cuts, -0.22, 0.18) * array
    return jnp.clip(array, min=-reach, max=reach).astype(held_as)


def gaussian_with(stream_key, shape, deviation, bound, pieces, heavy, held_as=jnp.bfloat16):
    array = deviation * jax.random.normal(stream_key, shape, jnp.float32)
    if pieces:
        array = array * level_of(stream_key, shape, pieces, -0.22, 0.18)
    return jnp.clip(with_spikes(array, jax.random.fold_in(stream_key, 3), *heavy), -bound, bound).astype(held_as)


def setup_inputs(seed: int = 0) -> dict:
    seeds = jax.random.split(jax.random.key(seed), 7)
    return {
        "tokens": normal_values(seeds[0], (TOKENS, D), 1.0, 6.0, ((0, 64), (1, 8))),
        "expert_ids": draw_expert_ids(jax.random.fold_in(seeds[6], 71), 0),
        "route_weight": jnp.clip(0.05 + 0.55 * jax.random.uniform(seeds[2], (TOKENS, TOP), jnp.float32) ** level_of(seeds[2], (TOKENS, TOP), ((0, 64),), -0.2, 0.2), 0.05, 0.6),
        "gate_weight": normal_values(seeds[3], (EXPERTS, FF, D), D ** -0.5, 0.09375, ((0, 64), (1, 8))),
        "up_weight": normal_values(seeds[4], (EXPERTS, FF, D), D ** -0.5, 0.09375, ((0, 64), (1, 8))),
        "down_weight": gaussian_with(seeds[5], (EXPERTS, FF, D), FF ** -0.5, 0.21875, ((0, 64), (1, 8)), (1, 2, 8, 2.0)),
    }


def project_rows(row_block, weight):
    return lax.dot_general(row_block, weight, (((1,), (1,)), ((), ())), preferred_element_type=jnp.float32)


def expert_block(row_block, w_gate, w_up, w_down):
    gate_val = project_rows(row_block, w_gate)
    up_val = project_rows(row_block, w_up)
    hidden = (jax.nn.silu(gate_val) * up_val).astype(jnp.bfloat16)
    group_width = hidden.shape[1] // N_TP
    summed = jnp.zeros((row_block.shape[0], w_down.shape[1]), jnp.float32)
    for number in range(N_TP):
        partial_value = jnp.dot(hidden[:, number * group_width:(number + 1) * group_width], w_down[number * group_width:(number + 1) * group_width], preferred_element_type=jnp.float32)
        partial_value = lax.optimization_barrier(partial_value.astype(jnp.bfloat16))
        summed = summed + partial_value.astype(jnp.float32)
    return summed.astype(jnp.bfloat16), hidden


def reference(tokens, expert_ids, route_weight, gate_weight, up_weight, down_weight):
    slot_count = N_EP * HOT_MOST
    flat_ids = expert_ids.reshape(N_EP, TOK_DEV * TOP)
    weights_flat = route_weight.reshape(N_EP, TOK_DEV * TOP)
    block_base = jnp.arange(N_EP, dtype=jnp.int32)[:, None]
    token_index = (block_base * TOK_DEV + jnp.arange(TOK_DEV * TOP, dtype=jnp.int32)[None, :] // TOP).astype(jnp.int32)

    def one_expert(carry, inputs):
        w_gate, w_up, w_down, expert = inputs
        chosen = (flat_ids == expert).astype(jnp.int32)
        rank_of = jnp.cumsum(chosen, axis=1) - 1
        target = jnp.where(chosen > 0, block_base * HOT_MOST + rank_of, slot_count).reshape(-1).astype(jnp.int32)
        source = jnp.zeros((slot_count,), jnp.int32).at[target].set(token_index.reshape(-1), mode="drop")
        scales = jnp.zeros((slot_count,), jnp.float32).at[target].set(weights_flat.reshape(-1), mode="drop")
        present = jnp.zeros((slot_count,), jnp.bool_).at[target].set(True, mode="drop")
        row_block = jnp.where(present[:, None], tokens[source], jnp.zeros((), jnp.bfloat16))
        result, hidden = expert_block(row_block, w_gate, w_up, w_down)
        carry = carry.at[source].add(result.astype(jnp.float32) * scales[:, None])
        peaks = jnp.stack([jnp.max(jnp.abs(row_block.astype(jnp.float32))), jnp.max(jnp.abs(hidden.astype(jnp.float32)))])
        return carry, peaks

    experts_axis = jnp.arange(EXPERTS, dtype=jnp.int32)
    summed, peaks = lax.scan(one_expert, jnp.zeros((TOKENS, D), jnp.float32), (gate_weight, up_weight, down_weight, experts_axis))
    return summed.astype(jnp.bfloat16), peaks.T
```

```python
import jax
import jax.numpy as jnp
from jax import lax
from jax.experimental import pallas as pl
from jax.experimental.pallas import tpu as pltpu
from jax.sharding import PartitionSpec as P

TOP = 8
SLOTS = 8
CORES = 2
BF = jnp.bfloat16
F32 = jnp.float32


def dot_nt(a, b):
    return lax.dot_general(a, b, (((1,), (1,)), ((), ())), preferred_element_type=F32)


def dot_nn(a, b):
    return lax.dot_general(a, b, (((1,), (0,)), ((), ())), preferred_element_type=F32)


def select_kernel(ids_ref, route_ref, tok_ref, out_ref, weight_ref):
    rows, slots = weight_ref.shape
    lane = lax.broadcasted_iota(jnp.int32, (rows, slots), 1)
    expert = lane // SLOTS
    ids = ids_ref[...]
    route = route_ref[...]
    named = jnp.zeros((rows, slots), F32)
    scale = jnp.zeros((rows, slots), F32)
    for k in range(TOP):
        hit = ids[:, k : k + 1] == expert
        named = jnp.where(hit, 1.0, named)
        scale = jnp.where(hit, route[:, k : k + 1], scale)
    before = (
        lax.broadcasted_iota(jnp.int32, (rows, rows), 1)
        < lax.broadcasted_iota(jnp.int32, (rows, rows), 0)
    )
    rank = dot_nn(before.astype(F32).astype(BF), named.astype(BF))
    taken = (named > 0.5) & (rank == (lane % SLOTS).astype(F32))
    weight_ref[...] = jnp.where(taken, scale, 0.0)
    pick = jnp.where(taken, 1.0, 0.0).astype(BF)
    out_ref[...] = lax.dot_general(
        pick, tok_ref[...], (((0,), (0,)), ((), ())), preferred_element_type=F32
    ).astype(BF)


def select_rows(ids, route, tokens, slots):
    rows, width = tokens.shape
    return pl.pallas_call(
        select_kernel,
        out_shape=(
            jax.ShapeDtypeStruct((slots, width), BF),
            jax.ShapeDtypeStruct((rows, slots), F32),
        ),
        name="select_rows",
    )(ids, route, tokens)


def early_kernel(
    order_ref, x0_ref, x1_ref, x2_ref, gate_ref, up_ref, gate_acc, up_acc, peak_ref
):
    step = pl.program_id(0)

    def add(x_ref, first):
        x = x_ref[...]
        gate = dot_nt(x, gate_ref[...])
        up = dot_nt(x, up_ref[...])
        peak = jnp.max(jnp.abs(x), axis=0, keepdims=True).astype(F32)
        if first:
            gate_acc[...] = gate
            up_acc[...] = up
            peak_ref[...] = peak
        else:
            gate_acc[...] += gate
            up_acc[...] += up
            peak_ref[...] = jnp.maximum(peak_ref[...], peak)

    @pl.when(step == 0)
    def _():
        add(x0_ref, True)

    @pl.when(step == 1)
    def _():
        add(x1_ref, False)

    @pl.when(step == 2)
    def _():
        add(x2_ref, False)


def early_project(order, chunks, gate, up):
    rows, width = chunks[0].shape
    units = gate.shape[0]
    whole = lambda shape: pl.BlockSpec(shape, lambda k, order: (0, 0))
    part = pl.BlockSpec((units, width), lambda k, order: (0, order[k]))
    return pl.pallas_call(
        early_kernel,
        grid_spec=pltpu.PrefetchScalarGridSpec(
            num_scalar_prefetch=1,
            grid=(3,),
            in_specs=[whole((rows, width))] * 3 + [part, part],
            out_specs=[whole((rows, units)), whole((rows, units)), whole((1, width))],
        ),
        out_shape=(
            jax.ShapeDtypeStruct((rows, units), F32),
            jax.ShapeDtypeStruct((rows, units), F32),
            jax.ShapeDtypeStruct((1, width), F32),
        ),
        cost_estimate=pl.CostEstimate(
            flops=12 * rows * width * units, transcendentals=0, bytes_accessed=12 * width * units
        ),
        name="early_project",
    )(order, *chunks, gate, up)


def late_kernel(order_ref, top_ref, low_ref, gate_ref, up_ref, gate_acc, up_acc, peak_in, hid_ref, peak_ref):
    half = top_ref.shape[0]
    peak = jnp.max(peak_in[...])
    for number, x_ref in enumerate((top_ref, low_ref)):
        rows = pl.ds(number * half, half)
        x = x_ref[...]
        gate = gate_acc[rows, :] + dot_nt(x, gate_ref[...])
        up = up_acc[rows, :] + dot_nt(x, up_ref[...])
        hid_ref[rows, :] = (gate / (1.0 + jnp.exp(-gate)) * up).astype(BF)
        peak = jnp.maximum(peak, jnp.max(jnp.abs(x).astype(F32)))
    peak_ref[...] = jnp.full(peak_ref.shape, peak, F32).astype(BF)


def late_project(order, top, low, gate, up, gate_acc, up_acc, peak_in, lanes):
    half, width = top.shape
    units = gate.shape[0]
    whole = lambda shape: pl.BlockSpec(shape, lambda k, order: (0, 0))
    part = pl.BlockSpec((units, width), lambda k, order: (0, order[3]))
    acc = whole((2 * half, units))
    return pl.pallas_call(
        late_kernel,
        grid_spec=pltpu.PrefetchScalarGridSpec(
            num_scalar_prefetch=1,
            grid=(1,),
            in_specs=[whole((half, width))] * 2 + [part, part, acc, acc, whole((1, width))],
            out_specs=[acc, whole((8, lanes))],
        ),
        out_shape=(
            jax.ShapeDtypeStruct((2 * half, units), BF),
            jax.ShapeDtypeStruct((8, lanes), BF),
        ),
        name="late_project",
    )(order, top, low, gate, up, gate_acc, up_acc, peak_in)


def down_kernel(order_ref, mine_ref, other_ref, down_ref, out_ref, column_ref):
    core = order_ref[4]
    parts, units, _ = down_ref.shape
    rows = out_ref.shape[0] // CORES
    in_peak = jnp.float32(0.0)
    hid_peak = jnp.float32(0.0)
    for number, ref in enumerate((mine_ref, other_ref)):
        total = None
        for part in range(parts):
            hidden = ref[pl.ds(0, rows), part * units : (part + 1) * units]
            value = dot_nn(hidden, down_ref[order_ref[part]])
            total = value if total is None else total + value
            hid_peak = jnp.maximum(hid_peak, jnp.max(jnp.abs(hidden).astype(F32)))
        in_peak = jnp.maximum(in_peak, jnp.max(ref[pl.ds(rows, 8), :].astype(F32)))
        place = core if number == 0 else 1 - core
        out_ref[pl.ds(pl.multiple_of(place * rows, rows), rows), :] = total.astype(BF)
    line = lax.broadcasted_iota(jnp.int32, column_ref.shape, 0)
    column_ref[...] = jnp.where(line == 0, in_peak, hid_peak)


def down_project(order, mine, other, down):
    parts, units, width = down.shape
    rows = mine.shape[0] - 8
    return pl.pallas_call(
        down_kernel,
        in_specs=[pl.BlockSpec(memory_space=pltpu.SMEM)] + [pl.BlockSpec(memory_space=pltpu.VMEM)] * 3,
        out_shape=(
            jax.ShapeDtypeStruct((CORES * rows, width), BF),
            jax.ShapeDtypeStruct((2, 1), F32),
        ),
        name="down_project",
    )(order, mine, other, down)


def combine_kernel(weight_ref, row_ref, out_ref):
    rest = weight_ref[...]
    total = None
    for _ in range(3):
        piece = rest.astype(BF)
        rest = rest - piece.astype(F32)
        value = dot_nn(piece, row_ref[...])
        total = value if total is None else total + value
    out_ref[...] = total.astype(BF)


def combine_rows(weight, rows):
    return pl.pallas_call(
        combine_kernel,
        out_shape=jax.ShapeDtypeStruct((weight.shape[0], rows.shape[1]), BF),
        name="combine_rows",
    )(weight, rows)


def body(tokens, expert_ids, route_weight, gate_weight, up_weight, down_weight):
    senders = lax.axis_size("ep")
    tp = lax.axis_size("tp")
    chips = tp // CORES
    index = lax.axis_index("tp")
    core = index % CORES
    place = index // CORES
    width = tokens.shape[1]
    unit = gate_weight.shape[1]

    def shift(array, step):
        return lax.ppermute(array, "tp", [(j, (j + CORES * step) % tp) for j in range(tp)])

    def partner(array):
        return lax.ppermute(array, "tp", [(j, j ^ 1) for j in range(tp)])

    def in_order(own, other, axis):
        return jnp.concatenate(
            [jnp.where(core == 0, own, other), jnp.where(core == 0, other, own)], axis=axis
        )

    def around(array):
        half = array.shape[0] // 2
        left = shift(array, 1)
        right = shift(array, -1)
        return left, right, shift(left[:half], 1), shift(right[half:], -1)

    outgoing, weight = select_rows(expert_ids, route_weight, tokens, senders * SLOTS)
    received = lax.all_to_all(
        outgoing.reshape(senders, SLOTS, width), "ep", split_axis=0, concat_axis=0, tiled=True
    ).reshape(senders * SLOTS, width)

    gate = in_order(gate_weight[0], partner(gate_weight[0]), 0)
    up = in_order(up_weight[0], partner(up_weight[0]), 0)
    down = lax.all_to_all(down_weight[0], "tp", split_axis=1, concat_axis=0, tiled=True)
    down = down.reshape(chips, CORES * unit, width)

    order = jnp.stack(
        [place, (place - 1) % chips, (place + 1) % chips, (place + 2) % chips, core]
    ).astype(jnp.int32)

    half = senders * SLOTS // CORES
    kept = lax.dynamic_slice_in_dim(received, core * half, half, 0)
    sent = lax.dynamic_slice_in_dim(received, (1 - core) * half, half, 0)
    rows = in_order(kept, partner(sent), 1)
    left, right, top, low = around(rows)
    gate_acc, up_acc, peak = early_project(order, (rows, left, right), gate, up)
    hidden, in_peak = late_project(
        order, top, low, gate, up, gate_acc, up_acc, peak, chips * CORES * unit
    )
    left, right, top, low = around(hidden)
    mine = jnp.concatenate(
        [
            jnp.concatenate([hidden, left, right, jnp.concatenate([top, low], axis=0)], axis=1),
            in_peak,
        ],
        axis=0,
    )
    out_rows, column = down_project(order, mine, partner(mine), down)
    returned = lax.all_to_all(
        out_rows.reshape(senders, SLOTS, width), "ep", split_axis=0, concat_axis=0, tiled=True
    ).reshape(senders * SLOTS, width)
    return combine_rows(weight, returned), column


def solution(mesh):
    return jax.shard_map(
        body,
        mesh=mesh,
        in_specs=(
            P("ep", "tp"),
            P("ep", None),
            P("ep", None),
            P("ep", "tp", None),
            P("ep", "tp", None),
            P("ep", "tp", None),
        ),
        out_specs=(P("ep", "tp"), P(None, "ep")),
        check_vma=False,
    )
```

```python
import jax
import jax.numpy as jnp
import numpy as np
from jax import lax
from jax.experimental import pallas as pl
from jax.experimental.pallas import tpu as pltpu
from jax.sharding import Mesh, PartitionSpec as P

TOP = 8
SLOTS = 8
CORES = 2
PAD = 8
BF = jnp.bfloat16
F32 = jnp.float32


IN_VMEM = pl.BlockSpec(memory_space=pltpu.VMEM)
IN_SMEM = pl.BlockSpec(memory_space=pltpu.SMEM)
ROOM = pltpu.CompilerParams(vmem_limit_bytes=28 << 20)


def local(array):
    return pltpu.with_memory_space_constraint(array, pltpu.VMEM)


def dot_nt(a, b):
    return lax.dot_general(a, b, (((1,), (1,)), ((), ())), preferred_element_type=F32)


def dot_nn(a, b):
    return lax.dot_general(a, b, (((1,), (0,)), ((), ())), preferred_element_type=F32)


def select_kernel(ids_ref, tok_ref, out_ref):
    slots = out_ref.shape[0]
    rows = tok_ref.shape[0]
    slot = lax.broadcasted_iota(jnp.int32, (slots, rows), 0)
    expert = slot // SLOTS
    named = jnp.zeros((slots, rows), F32)
    for k in range(TOP):
        named = jnp.where(ids_ref[k : k + 1, :] == expert, 1.0, named)
    before = (
        lax.broadcasted_iota(jnp.int32, (rows, rows), 0)
        < lax.broadcasted_iota(jnp.int32, (rows, rows), 1)
    )
    rank = dot_nn(named.astype(BF), before.astype(F32).astype(BF))
    taken = (named > 0.5) & (rank == (slot % SLOTS).astype(F32))
    pick = jnp.where(taken, 1.0, 0.0).astype(BF)
    out_ref[...] = dot_nn(pick, tok_ref[...]).astype(BF)


def select_rows(ids, tokens, slots):
    return pl.pallas_call(
        select_kernel,
        out_shape=jax.ShapeDtypeStruct((slots, tokens.shape[1]), BF),
        in_specs=[IN_VMEM] * 2,
        out_specs=IN_VMEM,
        compiler_params=ROOM,
        name="select_rows",
    )(ids, tokens)


def weigh_kernel(ids_ref, route_ref, weight_ref):
    rows, slots = weight_ref.shape
    lane = lax.broadcasted_iota(jnp.int32, (rows, slots), 1)
    expert = lane // SLOTS
    ids = ids_ref[...]
    route = route_ref[...]
    named = jnp.zeros((rows, slots), F32)
    scale = jnp.zeros((rows, slots), F32)
    for k in range(TOP):
        hit = ids[:, k : k + 1] == expert
        named = jnp.where(hit, 1.0, named)
        scale = jnp.where(hit, route[:, k : k + 1], scale)
    before = (
        lax.broadcasted_iota(jnp.int32, (rows, rows), 1)
        < lax.broadcasted_iota(jnp.int32, (rows, rows), 0)
    )
    rank = dot_nn(before.astype(F32).astype(BF), named.astype(BF))
    taken = (named > 0.5) & (rank == (lane % SLOTS).astype(F32))
    weight_ref[...] = jnp.where(taken, scale, 0.0)


def weigh_slots(ids, route, slots):
    return pl.pallas_call(
        weigh_kernel,
        out_shape=jax.ShapeDtypeStruct((ids.shape[0], slots), F32),
        compiler_params=ROOM,
        name="weigh_slots",
    )(ids, route)


def cut_kernel(order_ref, down_ref, *out_refs):
    own = order_ref[6]
    tp = len(out_refs)
    width = out_refs[0].shape[1]
    for step, out_ref in enumerate(out_refs):
        start = pl.multiple_of(((own + step) % tp) * width, width)
        out_ref[...] = down_ref[:, pl.ds(start, width)]


def cut_down(order, down, tp):
    unit, wide = down.shape
    return pl.pallas_call(
        cut_kernel,
        in_specs=[IN_SMEM, IN_VMEM],
        out_specs=[IN_VMEM] * tp,
        out_shape=[jax.ShapeDtypeStruct((unit, wide // tp), BF)] * tp,
        compiler_params=ROOM,
        name="cut_down",
    )(order, down)


def join_kernel(order_ref, got_ref, swap_ref, top_ref, low_ref):
    core = order_ref[4]
    half, width = top_ref.shape
    width = width // CORES
    start = pl.multiple_of(core * (2 * half), 2 * half)
    for number, ref in enumerate((top_ref, low_ref)):
        rows = pl.ds(start + number * half, half)
        ref[:, pl.ds(pl.multiple_of(core * width, width), width)] = got_ref[rows, :]
        ref[:, pl.ds(pl.multiple_of((1 - core) * width, width), width)] = swap_ref[
            pl.ds(number * half, half), :
        ]


def join_rows(order, received, swapped):
    half, width = swapped.shape[0] // 2, swapped.shape[1]
    return pl.pallas_call(
        join_kernel,
        in_specs=[IN_SMEM, IN_VMEM, IN_VMEM],
        out_specs=[IN_VMEM] * 2,
        out_shape=[jax.ShapeDtypeStruct((half, CORES * width), BF)] * 2,
        compiler_params=ROOM,
        name="join_rows",
    )(order, local(received), local(swapped))


def early_kernel(order_ref, *refs):
    pieces = refs[:6]
    gate_own, gate_other, up_own, up_other = refs[6:10]
    acc_ref, far_ref, peak_ref, x_ref, w_ref = refs[10:]
    core = order_ref[4]
    half, width = pieces[0].shape
    unit = gate_own.shape[0]
    own = pl.multiple_of(core * unit, unit)
    other = pl.multiple_of((1 - core) * unit, unit)

    def weights(target, chip):
        lanes = pl.ds(pl.multiple_of(chip * width, width), width)
        target[pl.ds(own, unit), :] = gate_own[:, lanes]
        target[pl.ds(other, unit), :] = gate_other[:, lanes]
        target[pl.ds(own + CORES * unit, unit), :] = up_own[:, lanes]
        target[pl.ds(other + CORES * unit, unit), :] = up_other[:, lanes]

    peak = None
    for number in range(3):
        x_ref[number, pl.ds(0, half), :] = pieces[2 * number][...]
        x_ref[number, pl.ds(half, half), :] = pieces[2 * number + 1][...]
        weights(w_ref.at[number], order_ref[number])
        x = x_ref[number]
        value = dot_nt(x, w_ref[number])
        if number == 0:
            acc_ref[...] = value
        else:
            acc_ref[...] += value
        top = jnp.max(jnp.abs(x).astype(F32), axis=0, keepdims=True)
        peak = top if peak is None else jnp.maximum(peak, top)
    peak_ref[...] = peak
    weights(far_ref, order_ref[3])


def early_project(order, pieces, weights):
    half, width = pieces[0].shape
    unit = weights[0].shape[0]
    wide = 2 * CORES * unit
    return pl.pallas_call(
        early_kernel,
        in_specs=[IN_SMEM] + [IN_VMEM] * 10,
        out_specs=[IN_VMEM] * 3,
        out_shape=(
            jax.ShapeDtypeStruct((2 * half, wide), F32),
            jax.ShapeDtypeStruct((wide, width), BF),
            jax.ShapeDtypeStruct((1, width), F32),
        ),
        scratch_shapes=[pltpu.VMEM((3, 2 * half, width), BF), pltpu.VMEM((3, wide, width), BF)],
        cost_estimate=pl.CostEstimate(
            flops=12 * half * width * wide, transcendentals=0, bytes_accessed=8 * width * wide
        ),
        compiler_params=ROOM,
        name="early_project",
    )(order, *(local(piece) for piece in pieces), *(local(array) for array in weights))


def late_kernel(top_ref, low_ref, far_ref, acc_ref, peak_in, hid_ref, x_ref):
    half = top_ref.shape[0]
    units = hid_ref.shape[1]
    x_ref[pl.ds(0, half), :] = top_ref[...]
    x_ref[pl.ds(half, half), :] = low_ref[...]
    x = x_ref[...]
    value = acc_ref[...] + dot_nt(x, far_ref[...])
    gate = value[:, :units]
    hid_ref[pl.ds(0, 2 * half), :] = (gate / (1.0 + jnp.exp(-gate)) * value[:, units:]).astype(BF)
    peak = jnp.maximum(jnp.max(peak_in[...]), jnp.max(jnp.abs(x).astype(F32)))
    hid_ref[pl.ds(2 * half, PAD), :] = jnp.full((PAD, units), peak, F32).astype(BF)


def late_project(top, low, far, acc, peak_in):
    half, width = top.shape
    units = far.shape[0] // 2
    return pl.pallas_call(
        late_kernel,
        in_specs=[IN_VMEM] * 5,
        out_specs=IN_VMEM,
        out_shape=jax.ShapeDtypeStruct((2 * half + PAD, units), BF),
        scratch_shapes=[pltpu.VMEM((2 * half, width), BF)],
        compiler_params=ROOM,
        name="late_project",
    )(*(local(array) for array in (top, low, far, acc, peak_in)))


def down_kernel(order_ref, mine_ref, other_ref, *refs):
    pieces, (out_ref, column_ref, w_ref) = refs[:-3], refs[-3:]
    core, own = order_ref[4], order_ref[6]
    tp = len(pieces)
    unit = pieces[0].shape[0]
    rows = out_ref.shape[0] // CORES
    for step, piece in enumerate(pieces):
        source = (own + tp - step) % tp
        w_ref[
            source // CORES, pl.ds(pl.multiple_of((source % CORES) * unit, unit), unit), :
        ] = piece[...]
    in_peak = jnp.float32(0.0)
    hid_peak = jnp.float32(0.0)
    for number, ref in enumerate((mine_ref, other_ref)):
        total = None
        for chip in range(tp // CORES):
            hidden = ref[chip, pl.ds(0, rows), :]
            value = dot_nn(hidden, w_ref[chip])
            total = value if total is None else total + value
            hid_peak = jnp.maximum(hid_peak, jnp.max(jnp.abs(hidden).astype(F32)))
        in_peak = jnp.maximum(in_peak, jnp.max(ref[0, pl.ds(rows, PAD), :].astype(F32)))
        place = core if number == 0 else 1 - core
        out_ref[pl.ds(pl.multiple_of(place * rows, rows), rows), :] = total.astype(BF)
    line = lax.broadcasted_iota(jnp.int32, column_ref.shape, 0)
    column_ref[...] = jnp.where(line == 0, in_peak, hid_peak)


def down_project(order, mine, other, pieces):
    tp = len(pieces)
    unit, width = pieces[0].shape
    chips, rows, units = mine.shape
    return pl.pallas_call(
        down_kernel,
        in_specs=[IN_SMEM] + [IN_VMEM] * (2 + tp),
        out_specs=[IN_VMEM] * 2,
        out_shape=(
            jax.ShapeDtypeStruct((CORES * (rows - PAD), width), BF),
            jax.ShapeDtypeStruct((2, 1), F32),
        ),
        scratch_shapes=[pltpu.VMEM((chips, units, width), BF)],
        compiler_params=ROOM,
        name="down_project",
    )(order, local(mine), local(other), *(local(piece) for piece in pieces))


def combine_kernel(weight_ref, row_ref, out_ref):
    rest = weight_ref[...]
    total = None
    for _ in range(3):
        piece = rest.astype(BF)
        rest = rest - piece.astype(F32)
        value = dot_nn(piece, row_ref[...])
        total = value if total is None else total + value
    out_ref[...] = total.astype(BF)


def combine_rows(weight, rows):
    return pl.pallas_call(
        combine_kernel,
        in_specs=[IN_VMEM] * 2,
        out_specs=IN_VMEM,
        out_shape=jax.ShapeDtypeStruct((weight.shape[0], rows.shape[1]), BF),
        compiler_params=ROOM,
        name="combine_rows",
    )(local(weight), local(rows))


def body(tokens, expert_ids, route_weight, gate_weight, up_weight, down_weight):
    senders = lax.axis_size("ep")
    chips = lax.axis_size("chip")
    tp = chips * CORES
    core = lax.axis_index("core")
    place = lax.axis_index("chip")
    width = tokens.shape[1]

    def shift(array, step):
        return lax.ppermute(array, "chip", [(j, (j + step) % chips) for j in range(chips)])

    def partner(array):
        return lax.ppermute(array, "core", [(j, 1 - j) for j in range(CORES)])

    def turn(array, step):
        return lax.ppermute(array, ("chip", "core"), [(j, (j + step) % tp) for j in range(tp)])

    lane = jnp.arange(8, dtype=jnp.int32)
    turns = jnp.array([0, chips - 1, 1, 2, 0, 0, 0, 0], jnp.int32)
    order = jnp.where(
        lane < 4, (place + turns) % chips, jnp.where(lane < 6, core, CORES * place + core)
    ).astype(jnp.int32)

    outgoing = select_rows(expert_ids.T, tokens, senders * SLOTS)
    received = lax.all_to_all(
        outgoing.reshape(senders, SLOTS, width), "ep", split_axis=0, concat_axis=0, tiled=True
    ).reshape(senders * SLOTS, width)

    gate_other = partner(gate_weight[0])
    up_other = partner(up_weight[0])
    cuts = cut_down(order, down_weight[0], tp)
    down = [cuts[0]] + [turn(cuts[step], step) for step in range(1, tp)]
    weight = weigh_slots(expert_ids, route_weight, senders * SLOTS)
    received, gate_other, up_other, weight, *down = lax.optimization_barrier(
        (received, gate_other, up_other, weight, *down)
    )

    half = senders * SLOTS // CORES
    sent = lax.dynamic_slice_in_dim(received, (1 - core) * half, half, 0)
    top, low = join_rows(order, received, partner(sent))
    left_top, right_low = shift(top, 1), shift(low, -1)
    left_low, right_top = shift(low, 1), shift(top, -1)
    far_top, far_low = shift(left_top, 1), shift(right_low, -1)
    acc, far, peak = early_project(
        order,
        (top, low, left_top, left_low, right_top, right_low),
        (gate_weight[0], gate_other, up_weight[0], up_other),
    )
    hidden = late_project(far_top, far_low, far, acc, peak)
    mine = lax.all_gather(hidden, "chip", axis=0)
    out_rows, column = down_project(order, mine, partner(mine), down)
    returned = lax.all_to_all(
        out_rows.reshape(senders, SLOTS, width), "ep", split_axis=0, concat_axis=0, tiled=True
    ).reshape(senders * SLOTS, width)
    return combine_rows(weight, returned), column


def solution(mesh):
    devices = np.asarray(mesh.devices)
    fine = Mesh(
        devices.reshape(devices.shape[0], devices.shape[1] // CORES, CORES), ("ep", "chip", "core")
    )
    tp = ("chip", "core")
    return jax.shard_map(
        body,
        mesh=fine,
        in_specs=(
            P("ep", tp),
            P("ep", None),
            P("ep", None),
            P("ep", tp, None),
            P("ep", tp, None),
            P("ep", tp, None),
        ),
        out_specs=(P("ep", tp), P(None, "ep")),
        check_vma=False,
    )
```

```python
import jax
import jax.numpy as jnp
import numpy as np
from jax import lax
from jax.experimental import pallas as pl
from jax.experimental.pallas import tpu as pltpu
from jax.sharding import Mesh, PartitionSpec as P

TOP = 8
SLOTS = 8
CORES = 2
X = 4
LANES = 128
BF = jnp.bfloat16
F32 = jnp.float32


IN_VMEM = pl.BlockSpec(memory_space=pltpu.VMEM)
IN_SMEM = pl.BlockSpec(memory_space=pltpu.SMEM)
ROOM = pltpu.CompilerParams(vmem_limit_bytes=24 << 20)


def local(array):
    return pltpu.with_memory_space_constraint(array, pltpu.VMEM)


def dot_nt(a, b):
    return lax.dot_general(a, b, (((1,), (1,)), ((), ())), preferred_element_type=F32)


def dot_nn(a, b):
    return lax.dot_general(a, b, (((1,), (0,)), ((), ())), preferred_element_type=F32)


def iota(shape, axis):
    return lax.broadcasted_iota(jnp.int32, shape, axis)


def call(kernel, name, order, inputs, out_shape, scratch=(), cost=None):
    single = isinstance(out_shape, jax.ShapeDtypeStruct)
    specs = ([] if order is None else [IN_SMEM]) + [IN_VMEM] * len(inputs)
    run = pl.pallas_call(
        kernel,
        in_specs=specs,
        out_specs=IN_VMEM if single else [IN_VMEM] * len(out_shape),
        out_shape=out_shape,
        scratch_shapes=list(scratch),
        compiler_params=ROOM,
        cost_estimate=cost,
        name=name,
    )
    return run(*(() if order is None else (order,)), *inputs)


def pack_kernel(order_ref, ids_ref, route_ref, tok_ref, out_ref):
    planes, height, _ = out_ref.shape
    rows, width = tok_ref.shape
    for group in range(width // LANES):
        piece = tok_ref[:, group * LANES : (group + 1) * LANES]
        for plane in range(planes):
            out_ref[plane, pl.ds(group * rows, rows), :] = piece
    lines = planes * 2 * X
    line = iota((lines, rows), 0)
    expert = (line % X) * planes + line // (2 * X)
    scale = jnp.zeros((lines, rows), F32)
    for k in range(TOP):
        scale = jnp.where(ids_ref[k : k + 1, :] == expert, route_ref[k : k + 1, :], scale)
    high = scale.astype(BF).astype(F32)
    value = jnp.where((line // X) % 2 == 0, high, scale - high).astype(BF)
    first = (order_ref[5] * rows) % LANES
    spread = (iota((rows, LANES), 1) == iota((rows, LANES), 0) + first).astype(F32).astype(BF)
    info = dot_nn(value, spread).reshape(planes, 2 * X, LANES)
    out_ref[:, pl.ds(height - 2 * X, 2 * X), :] = info.astype(BF)


def route_tables(got_ref, rows):
    planes, height, _ = got_ref.shape
    span = LANES // rows
    parts = []
    for start in range(0, planes, span):
        total = None
        for plane in range(start, start + span):
            part = got_ref[plane, pl.ds(height - 2 * X, 2 * X), :].astype(F32)
            total = part if total is None else total + part
        parts.append(total)
    table = jnp.concatenate(parts, axis=1)
    tokens = planes * rows
    left, right = iota((tokens, tokens), 0), iota((tokens, tokens), 1)
    before = ((left // rows == right // rows) & (left < right)).astype(F32).astype(BF)
    rank = dot_nn((table > 0.0).astype(F32).astype(BF), before)
    return table, rank


def taken_rows(table, rank, j, rows):
    tokens = table.shape[1]
    count = tokens // rows * SLOTS
    row, token = iota((count, tokens), 0), iota((count, tokens), 1)
    return (
        (table[j : j + 1, :] > 0.0)
        & (row // SLOTS == token // rows)
        & (rank[j : j + 1, :] == (row % SLOTS).astype(F32))
    )


def pick_kernel(got_ref, out_ref, tok_ref, pick_ref):
    planes, height, _ = got_ref.shape
    groups = tok_ref.shape[1] // LANES
    rows = (height - 2 * X) // groups
    table, rank = route_tables(got_ref, rows)
    for plane in range(planes):
        for group in range(groups):
            tok_ref[pl.ds(plane * rows, rows), group * LANES : (group + 1) * LANES] = got_ref[
                plane, pl.ds(group * rows, rows), :
            ]
    count = planes * SLOTS
    for j in range(X):
        pick_ref[pl.ds(j * count, count), :] = (
            taken_rows(table, rank, j, rows).astype(F32).astype(BF)
        )
    out_ref[...] = dot_nn(pick_ref[...], tok_ref[...]).astype(BF).reshape(out_ref.shape)


def weigh_kernel(got_ref, high_ref, low_ref):
    planes = got_ref.shape[0]
    rows = high_ref.shape[0] // planes
    table, rank = route_tables(got_ref, rows)
    count = planes * SLOTS
    for j in range(X):
        taken = taken_rows(table, rank, j, rows)
        for ref, line in ((high_ref, j), (low_ref, X + j)):
            value = jnp.where(taken, table[line : line + 1, :], 0.0)
            ref[:, j * count : (j + 1) * count] = value.T.astype(BF)


def join_kernel(got_ref, out_ref):
    _, rows, width = got_ref.shape
    for x in range(X):
        for core in range(CORES):
            out_ref[pl.ds(x * rows, rows), core * width : (core + 1) * width] = got_ref[
                x * CORES + core
            ]


def first_kernel(
    order_ref, x_ref, gate_own, gate_other, up_own, up_other, acc_ref, rest_ref, peak_ref, w_ref
):
    core = order_ref[4]
    width = x_ref.shape[1]
    unit = gate_own.shape[0]
    own = pl.multiple_of(core * unit, unit)
    other = pl.multiple_of((1 - core) * unit, unit)

    def weights(target, chip):
        lanes = pl.ds(pl.multiple_of(chip * width, width), width)
        target[pl.ds(own, unit), :] = gate_own[:, lanes]
        target[pl.ds(other, unit), :] = gate_other[:, lanes]
        target[pl.ds(own + CORES * unit, unit), :] = up_own[:, lanes]
        target[pl.ds(other + CORES * unit, unit), :] = up_other[:, lanes]

    weights(w_ref, order_ref[0])
    x = x_ref[...]
    acc_ref[...] = dot_nt(x, w_ref[...])
    peak_ref[...] = jnp.max(jnp.abs(x).astype(F32), axis=0, keepdims=True)
    for number in range(3):
        weights(rest_ref.at[number], order_ref[number + 1])


def near_kernel(left_ref, right_ref, rest_ref, acc_in, peak_in, acc_ref, peak_ref):
    left, right = left_ref[...], right_ref[...]
    acc_ref[...] = acc_in[...] + dot_nt(left, rest_ref[0]) + dot_nt(right, rest_ref[1])
    peak = jnp.max(jnp.maximum(jnp.abs(left), jnp.abs(right)).astype(F32), axis=0, keepdims=True)
    peak_ref[...] = jnp.maximum(peak_in[...], peak)


def far_kernel(top_ref, low_ref, rest_ref, acc_ref, peak_in, hid_ref, peak_ref, x_ref):
    half = top_ref.shape[0]
    units = hid_ref.shape[1]
    x_ref[pl.ds(0, half), :] = top_ref[...]
    x_ref[pl.ds(half, half), :] = low_ref[...]
    x = x_ref[...]
    value = acc_ref[...] + dot_nt(x, rest_ref[2])
    gate = value[:, :units]
    hid_ref[...] = (gate / (1.0 + jnp.exp(-gate)) * value[:, units:]).astype(BF)
    peak = jnp.maximum(jnp.max(peak_in[...]), jnp.max(jnp.abs(x).astype(F32)))
    peak_ref[...] = jnp.full(peak_ref.shape, peak, F32)


def cut_kernel(order_ref, down_ref, *out_refs):
    width = out_refs[0].shape[1]
    for number, out_ref in enumerate(out_refs):
        start = pl.multiple_of(order_ref[number] * width, width)
        out_ref[...] = down_ref[:, pl.ds(start, width)]


def stack_kernel(order_ref, *refs):
    for number, piece in enumerate(refs[:-1]):
        refs[-1][order_ref[number]] = piece[...]


def pair_kernel(order_ref, own_ref, other_ref, out_ref):
    chips, unit, _ = own_ref.shape
    core = order_ref[4]
    for chip in range(chips):
        base = chip * CORES * unit
        out_ref[pl.ds(pl.multiple_of(base + core * unit, unit), unit), :] = own_ref[chip]
        out_ref[pl.ds(pl.multiple_of(base + (1 - core) * unit, unit), unit), :] = other_ref[chip]


def down_kernel(hid_ref, down_ref, peak_in, out_ref, peak_ref, h_ref):
    chips, _, units = hid_ref.shape
    for chip in range(chips):
        h_ref[:, chip * units : (chip + 1) * units] = hid_ref[chip]
    hidden = h_ref[...]
    value = dot_nn(hidden, down_ref[...]).astype(BF)
    _, rows, width = out_ref.shape
    for x in range(X):
        for core in range(CORES):
            out_ref[x * CORES + core] = value[
                x * rows : (x + 1) * rows, core * width : (core + 1) * width
            ]
    peak = jnp.max(jnp.abs(hidden).astype(F32))
    peak_ref[...] = jnp.where(iota(peak_ref.shape, 0) == 0, peak_in[...], peak)


def combine_kernel(high_ref, low_ref, row_ref, out_ref):
    rows = row_ref[...].reshape(high_ref.shape[1], row_ref.shape[2])
    value = dot_nn(high_ref[...], rows) + dot_nn(low_ref[...], rows)
    out_ref[...] = value.astype(BF).reshape(out_ref.shape)


def total_kernel(part_ref, out_ref):
    total = part_ref[0].astype(F32)
    for plane in range(1, part_ref.shape[0]):
        total = total + part_ref[plane].astype(F32)
    out_ref[...] = total.astype(BF)


def body(tokens, expert_ids, route_weight, gate_weight, up_weight, down_weight):
    planes = lax.axis_size("z")
    chips = lax.axis_size("chip")
    core = lax.axis_index("core")
    place = lax.axis_index("chip")
    rows, width = tokens.shape
    unit, wide = gate_weight.shape[1:]
    chunk = CORES * width
    units = CORES * unit
    kept = X * planes * SLOTS // CORES
    shaped = jax.ShapeDtypeStruct

    def shift(array, step):
        return lax.ppermute(array, "chip", [(j, (j + step) % chips) for j in range(chips)])

    def partner(array):
        return lax.ppermute(array, "core", [(j, 1 - j) for j in range(CORES)])

    lane = jnp.arange(8, dtype=jnp.int32)
    turns = jnp.array([0, chips - 1, 1, 2, 0, 0, 0, 0], jnp.int32)
    order = jnp.where(
        lane < 4, (place + turns) % chips, jnp.where(lane == 4, core, lax.axis_index("z"))
    ).astype(jnp.int32)

    height = width // LANES * rows + 2 * X
    packed = call(
        pack_kernel,
        "pack_tokens",
        order,
        (expert_ids.T, route_weight.T, tokens),
        shaped((planes, height, LANES), BF),
    )
    plane_rows = lax.all_to_all(packed, "z", split_axis=0, concat_axis=0, tiled=True)

    gate_other = partner(gate_weight[0])
    up_other = partner(up_weight[0])
    cuts = call(
        cut_kernel, "cut_down", order, (down_weight[0],), [shaped((unit, chunk), BF)] * chips
    )
    pieces = [cuts[0], shift(cuts[2], 1), shift(cuts[1], -1), shift(cuts[3], 2)]

    sent = call(
        pick_kernel,
        "pick_rows",
        None,
        (local(plane_rows),),
        shaped((X * CORES, kept // X, width), BF),
        (
            pltpu.VMEM((planes * rows, width), BF),
            pltpu.VMEM((X * planes * SLOTS, planes * rows), BF),
        ),
    )
    received = lax.all_to_all(sent, ("x", "core"), split_axis=0, concat_axis=0, tiled=True)
    received, gate_other, up_other, *pieces = lax.optimization_barrier(
        (received, gate_other, up_other, *pieces)
    )

    x = call(join_kernel, "join_rows", None, (local(received),), shaped((kept, chunk), BF))
    left, right = shift(x, 1), shift(x, -1)
    stacked = call(
        stack_kernel,
        "stack_down",
        order,
        tuple(local(piece) for piece in pieces),
        shaped((chips, unit, chunk), BF),
    )
    down = call(
        pair_kernel,
        "pair_down",
        order,
        (local(stacked), local(partner(stacked))),
        shaped((chips * units, chunk), BF),
    )
    high, low = call(
        weigh_kernel,
        "weigh_rows",
        None,
        (local(plane_rows),),
        [shaped((planes * rows, X * planes * SLOTS), BF)] * 2,
    )
    acc, rest, peak = call(
        first_kernel,
        "first_chunk",
        order,
        tuple(local(a) for a in (x, gate_weight[0], gate_other, up_weight[0], up_other)),
        [
            shaped((kept, 2 * units), F32),
            shaped((3, 2 * units, chunk), BF),
            shaped((1, chunk), F32),
        ],
        (pltpu.VMEM((2 * units, chunk), BF),),
        pl.CostEstimate(
            flops=4 * kept * chunk * units, transcendentals=0, bytes_accessed=16 * units * chunk
        ),
    )
    far_top, far_low = shift(left[: kept // 2], 1), shift(right[kept // 2 :], -1)
    acc, peak = call(
        near_kernel,
        "near_chunks",
        None,
        tuple(local(a) for a in (left, right, rest, acc, peak)),
        [shaped((kept, 2 * units), F32), shaped((1, chunk), F32)],
        cost=pl.CostEstimate(
            flops=8 * kept * chunk * units, transcendentals=0, bytes_accessed=8 * units * chunk
        ),
    )
    hidden, peak = call(
        far_kernel,
        "far_chunk",
        None,
        tuple(local(a) for a in (far_top, far_low, rest, acc, peak)),
        [shaped((kept, units), BF), shaped((8, LANES), F32)],
        (pltpu.VMEM((kept, chunk), BF),),
    )
    gathered = lax.all_gather(hidden, "chip", axis=0)
    outputs, peak = call(
        down_kernel,
        "down_rows",
        None,
        tuple(local(a) for a in (gathered, down, peak)),
        [shaped((X * CORES, kept // X, width), BF), shaped((8, LANES), F32)],
        (pltpu.VMEM((kept, chips * units), BF),),
    )
    returned = lax.all_to_all(outputs, ("x", "core"), split_axis=0, concat_axis=0, tiled=True)
    column = jnp.maximum(peak, partner(peak))[:2, :1]
    sums = call(
        combine_kernel,
        "combine_rows",
        None,
        tuple(local(a) for a in (high, low, returned)),
        shaped((planes, rows, width), BF),
    )
    parts = lax.all_to_all(sums, "z", split_axis=0, concat_axis=0, tiled=True)
    moe_out = call(total_kernel, "total_planes", None, (local(parts),), shaped((rows, width), BF))
    return moe_out, column


def solution(mesh):
    devices = np.asarray(mesh.devices)
    ep, tp = devices.shape
    fine = Mesh(
        devices.reshape(X, ep // X, tp // CORES, CORES), ("x", "z", "chip", "core")
    )
    ep, tp = ("x", "z"), ("chip", "core")
    return jax.shard_map(
        body,
        mesh=fine,
        in_specs=(
            P(ep, tp),
            P(ep, None),
            P(ep, None),
            P(ep, tp, None),
            P(ep, tp, None),
            P(ep, tp, None),
        ),
        out_specs=(P(ep, tp), P(None, ep)),
        check_vma=False,
    )
```

```python
import jax
import jax.numpy as jnp
import numpy as np
from jax import lax
from jax.experimental import pallas as pl
from jax.experimental.pallas import tpu as pltpu
from jax.sharding import Mesh, PartitionSpec as P


TOP = 8
SLOTS = 8
CORES = 2
X = 4
LANES = 128
BF = jnp.bfloat16
F32 = jnp.float32


IN_VMEM = pl.BlockSpec(memory_space=pltpu.VMEM)
IN_PLACE = pl.BlockSpec(memory_space=pltpu.HBM)
IN_SMEM = pl.BlockSpec(memory_space=pltpu.SMEM)
ROOM = pltpu.CompilerParams(vmem_limit_bytes=24 << 20)


def local(array):
    return pltpu.with_memory_space_constraint(array, pltpu.VMEM)


def remote(array):
    return pltpu.with_memory_space_constraint(array, pltpu.HBM)


def dot_nt(a, b):
    return lax.dot_general(a, b, (((1,), (1,)), ((), ())), preferred_element_type=F32)


def dot_nn(a, b):
    return lax.dot_general(a, b, (((1,), (0,)), ((), ())), preferred_element_type=F32)


def iota(shape, axis):
    return lax.broadcasted_iota(jnp.int32, shape, axis)


def call(kernel, order, inputs, out_shape, scratch=(), cost=None):
    single = isinstance(out_shape, jax.ShapeDtypeStruct)
    specs = ([] if order is None else [IN_SMEM]) + [IN_VMEM] * len(inputs)
    run = pl.pallas_call(
        kernel,
        in_specs=specs,
        out_specs=IN_VMEM if single else [IN_VMEM] * len(out_shape),
        out_shape=out_shape,
        scratch_shapes=list(scratch),
        compiler_params=ROOM,
        cost_estimate=cost,
    )
    return run(*(() if order is None else (order,)), *inputs)


def pack_kernel(ids_hbm, route_hbm, tok_hbm, out_ref, ids_ref, route_ref, tok_ref, sems):
    copies = [
        pltpu.make_async_copy(source, target, sems.at[number])
        for number, (source, target) in enumerate(
            ((ids_hbm, ids_ref), (route_hbm, route_ref), (tok_hbm, tok_ref))
        )
    ]
    for copy in copies:
        copy.start()
    for copy in copies:
        copy.wait()
    planes, height, _ = out_ref.shape
    rows, width = tok_ref.shape
    for group in range(width // LANES):
        piece = tok_ref[:, group * LANES : (group + 1) * LANES]
        for plane in range(planes):
            out_ref[plane, pl.ds(group * rows, rows), :] = piece
    lines = planes * 2 * X
    line = iota((lines, rows), 0)
    expert = (line % X) * planes + line // (2 * X)
    scale = jnp.zeros((lines, rows), F32)
    for k in range(TOP):
        scale = jnp.where(ids_ref[k : k + 1, :] == expert, route_ref[k : k + 1, :], scale)
    high = scale.astype(BF).astype(F32)
    value = jnp.where((line // X) % 2 == 0, high, scale - high).astype(BF)
    spread = (iota((rows, LANES), 1) == iota((rows, LANES), 0)).astype(F32).astype(BF)
    info = dot_nn(value, spread).reshape(planes, 2 * X, LANES)
    out_ref[:, pl.ds(height - 2 * X, 2 * X), :] = info.astype(BF)


def pack_tokens(ids, route, tokens, planes):
    rows, width = tokens.shape
    height = width // LANES * rows + 2 * X
    return pl.pallas_call(
        pack_kernel,
        in_specs=[IN_PLACE] * 3,
        out_specs=IN_VMEM,
        out_shape=jax.ShapeDtypeStruct((planes, height, LANES), BF),
        scratch_shapes=[
            pltpu.VMEM(ids.shape, ids.dtype),
            pltpu.VMEM(route.shape, route.dtype),
            pltpu.VMEM(tokens.shape, tokens.dtype),
            pltpu.SemaphoreType.DMA((3,)),
        ],
        compiler_params=ROOM,
        name="pack_tokens",
    )(remote(ids), remote(route), remote(tokens))


def route_tables(got_ref, rows):
    planes, height, _ = got_ref.shape
    span = LANES // rows
    parts = []
    for start in range(0, planes, span):
        total = None
        for plane in range(start, start + span):
            part = got_ref[plane, pl.ds(height - 2 * X, 2 * X), :].astype(F32)
            if plane > start:
                part = pltpu.roll(part, (plane - start) * rows, 1)
            total = part if total is None else total + part
        parts.append(total)
    table = jnp.concatenate(parts, axis=1)
    tokens = planes * rows
    left, right = iota((tokens, tokens), 0), iota((tokens, tokens), 1)
    before = ((left // rows == right // rows) & (left < right)).astype(F32).astype(BF)
    rank = dot_nn((table > 0.0).astype(F32).astype(BF), before)
    return table, rank


def taken_rows(table, rank, j, rows):
    tokens = table.shape[1]
    count = tokens // rows * SLOTS
    row, token = iota((count, tokens), 0), iota((count, tokens), 1)
    return (
        (table[j : j + 1, :] > 0.0)
        & (row // SLOTS == token // rows)
        & (rank[j : j + 1, :] == (row % SLOTS).astype(F32))
    )


def pick_kernel(got_ref, out_ref, tok_ref, pick_ref):
    planes, height, _ = got_ref.shape
    groups = tok_ref.shape[1] // LANES
    rows = (height - 2 * X) // groups
    table, rank = route_tables(got_ref, rows)
    for plane in range(planes):
        for group in range(groups):
            tok_ref[pl.ds(plane * rows, rows), group * LANES : (group + 1) * LANES] = got_ref[
                plane, pl.ds(group * rows, rows), :
            ]
    count = planes * SLOTS
    for j in range(X):
        pick_ref[pl.ds(j * count, count), :] = (
            taken_rows(table, rank, j, rows).astype(F32).astype(BF)
        )
    out_ref[...] = dot_nn(pick_ref[...], tok_ref[...]).astype(BF).reshape(out_ref.shape)


def weigh_kernel(got_ref, high_ref, low_ref):
    planes = got_ref.shape[0]
    rows = high_ref.shape[0] // planes
    table, rank = route_tables(got_ref, rows)
    count = planes * SLOTS
    for j in range(X):
        taken = taken_rows(table, rank, j, rows)
        for ref, line in ((high_ref, j), (low_ref, X + j)):
            value = jnp.where(taken, table[line : line + 1, :], 0.0)
            ref[:, j * count : (j + 1) * count] = value.T.astype(BF)


def join_kernel(got_ref, top_ref, low_ref):
    _, rows, width = got_ref.shape
    half = X // 2
    for x in range(X):
        ref = top_ref if x < half else low_ref
        for core in range(CORES):
            ref[pl.ds((x % half) * rows, rows), core * width : (core + 1) * width] = got_ref[
                x * CORES + core
            ]


def arrange_kernel(order_ref, gate_own, gate_other, up_own, up_other, out_ref):
    core = order_ref[4]
    chips, _, width = out_ref.shape
    unit = gate_own.shape[0]
    own = pl.multiple_of(core * unit, unit)
    other = pl.multiple_of((1 - core) * unit, unit)
    for number in range(chips):
        lanes = pl.ds(pl.multiple_of(order_ref[number] * width, width), width)
        out_ref[number, pl.ds(own, unit), :] = gate_own[:, lanes]
        out_ref[number, pl.ds(other, unit), :] = gate_other[:, lanes]
        out_ref[number, pl.ds(own + CORES * unit, unit), :] = up_own[:, lanes]
        out_ref[number, pl.ds(other + CORES * unit, unit), :] = up_other[:, lanes]


def near_kernel(*refs):
    pieces, (table_hbm, acc_ref, peak_ref, last_ref, x_ref, w_ref, sems) = refs[:6], refs[6:]
    half = pieces[0].shape[0]
    copies = [
        pltpu.make_async_copy(
            table_hbm.at[number], w_ref.at[number] if number < 3 else last_ref, sems.at[number]
        )
        for number in range(4)
    ]
    for copy in copies:
        copy.start()
    peak = None
    total = None
    for number in range(3):
        x_ref[number, pl.ds(0, half), :] = pieces[2 * number][...]
        x_ref[number, pl.ds(half, half), :] = pieces[2 * number + 1][...]
        x = x_ref[number]
        copies[number].wait()
        value = dot_nt(x, w_ref[number])
        total = value if total is None else total + value
        high = jnp.max(jnp.abs(x).astype(F32), axis=0, keepdims=True)
        peak = high if peak is None else jnp.maximum(peak, high)
    acc_ref[...] = total
    peak_ref[...] = peak
    copies[3].wait()


def near_chunks(pieces, table):
    half, width = pieces[0].shape
    wide = table.shape[1]
    return pl.pallas_call(
        near_kernel,
        in_specs=[IN_VMEM] * 6 + [IN_PLACE],
        out_specs=[IN_VMEM] * 3,
        out_shape=[
            jax.ShapeDtypeStruct((2 * half, wide), F32),
            jax.ShapeDtypeStruct((1, width), F32),
            jax.ShapeDtypeStruct((wide, width), BF),
        ],
        scratch_shapes=[
            pltpu.VMEM((3, 2 * half, width), BF),
            pltpu.VMEM((3, wide, width), BF),
            pltpu.SemaphoreType.DMA((4,)),
        ],
        compiler_params=ROOM,
        cost_estimate=pl.CostEstimate(
            flops=12 * half * width * wide, transcendentals=0, bytes_accessed=8 * width * wide
        ),
        name="near_chunks",
    )(*(local(piece) for piece in pieces), remote(table))


def far_kernel(top_ref, low_ref, table_ref, acc_ref, peak_in, hid_ref, peak_ref, x_ref):
    half = top_ref.shape[0]
    units = hid_ref.shape[1]
    x_ref[pl.ds(0, half), :] = top_ref[...]
    x_ref[pl.ds(half, half), :] = low_ref[...]
    x = x_ref[...]
    value = acc_ref[...] + dot_nt(x, table_ref[...])
    gate = value[:, :units]
    hid_ref[...] = (gate / (1.0 + jnp.exp(-gate)) * value[:, units:]).astype(BF)
    peak = jnp.maximum(jnp.max(peak_in[...]), jnp.max(jnp.abs(x).astype(F32)))
    peak_ref[...] = jnp.full(peak_ref.shape, peak, F32)


def cut_kernel(order_ref, down_ref, *out_refs):
    width = out_refs[0].shape[1]
    for number, out_ref in enumerate(out_refs):
        start = pl.multiple_of(order_ref[number] * width, width)
        out_ref[...] = down_ref[:, pl.ds(start, width)]


def stack_kernel(order_ref, *refs):
    for number, piece in enumerate(refs[:-1]):
        refs[-1][order_ref[number]] = piece[...]


def pair_kernel(order_ref, own_ref, other_ref, out_ref):
    chips, unit, _ = own_ref.shape
    core = order_ref[4]
    for chip in range(chips):
        base = chip * CORES * unit
        out_ref[pl.ds(pl.multiple_of(base + core * unit, unit), unit), :] = own_ref[chip]
        out_ref[pl.ds(pl.multiple_of(base + (1 - core) * unit, unit), unit), :] = other_ref[chip]


def down_kernel(hid_ref, down_ref, peak_in, out_ref, peak_ref, h_ref):
    chips, _, units = hid_ref.shape
    for chip in range(chips):
        h_ref[:, chip * units : (chip + 1) * units] = hid_ref[chip]
    hidden = h_ref[...]
    value = dot_nn(hidden, down_ref[...]).astype(BF)
    _, rows, width = out_ref.shape
    for x in range(X):
        for core in range(CORES):
            out_ref[x * CORES + core] = value[
                x * rows : (x + 1) * rows, core * width : (core + 1) * width
            ]
    peak = jnp.max(jnp.abs(hidden).astype(F32))
    peak_ref[...] = jnp.where(iota(peak_ref.shape, 0) == 0, peak_in[...], peak)


def combine_kernel(high_ref, low_ref, row_ref, out_ref):
    rows = row_ref[...].reshape(high_ref.shape[1], row_ref.shape[2])
    value = dot_nn(high_ref[...], rows) + dot_nn(low_ref[...], rows)
    out_ref[...] = value.astype(BF).reshape(out_ref.shape)


def total_kernel(part_ref, out_ref):
    total = part_ref[0].astype(F32)
    for plane in range(1, part_ref.shape[0]):
        total = total + part_ref[plane].astype(F32)
    out_ref[...] = total.astype(BF)


def layer(tokens, expert_ids, route_weight, gate_weight, up_weight, down_weight):
    planes = lax.axis_size("z")
    chips = lax.axis_size("chip")
    core = lax.axis_index("core")
    place = lax.axis_index("chip")
    rows, width = tokens.shape
    unit, _ = gate_weight.shape[1:]
    chunk = CORES * width
    units = CORES * unit
    kept = X * planes * SLOTS // CORES
    shaped = jax.ShapeDtypeStruct

    def shift(array, step):
        return lax.ppermute(array, "chip", [(j, (j + step) % chips) for j in range(chips)])

    def partner(array):
        return lax.ppermute(array, "core", [(j, 1 - j) for j in range(CORES)])

    lane = jnp.arange(8, dtype=jnp.int32)
    turns = jnp.array([0, chips - 1, 1, 2, 0, 0, 0, 0], jnp.int32)
    order = jnp.where(
        lane < 4, (place + turns) % chips, jnp.where(lane == 4, core, lax.axis_index("z"))
    ).astype(jnp.int32)

    packed = pack_tokens(expert_ids.T, route_weight.T, tokens, planes)
    plane_rows = lax.all_to_all(packed, "z", split_axis=0, concat_axis=0, tiled=True)

    gate_other = partner(gate_weight[0])
    up_other = partner(up_weight[0])
    cuts = call(cut_kernel, order, (down_weight[0],), [shaped((unit, chunk), BF)] * chips)
    pieces = [cuts[0], shift(cuts[2], 1), shift(cuts[1], -1), shift(cuts[3], 2)]
    table = call(
        arrange_kernel,
        order,
        tuple(local(a) for a in (gate_weight[0], gate_other, up_weight[0], up_other)),
        shaped((chips, 2 * units, chunk), BF),
    )

    sent = call(
        pick_kernel,
        None,
        (local(plane_rows),),
        shaped((X * CORES, kept // X, width), BF),
        (
            pltpu.VMEM((planes * rows, width), BF),
            pltpu.VMEM((X * planes * SLOTS, planes * rows), BF),
        ),
    )
    received = lax.all_to_all(sent, ("x", "core"), split_axis=0, concat_axis=0, tiled=True)
    stacked = call(
        stack_kernel,
        order,
        tuple(remote(piece) for piece in pieces),
        shaped((chips, unit, chunk), BF),
    )
    stacked_other = partner(stacked)
    high, low = call(
        weigh_kernel,
        None,
        (local(plane_rows),),
        [shaped((planes * rows, X * planes * SLOTS), BF)] * 2,
    )

    top, bottom = call(join_kernel, None, (local(received),), [shaped((kept // 2, chunk), BF)] * 2)
    left_top, right_low = shift(top, 1), shift(bottom, -1)
    left_low, right_top = shift(bottom, 1), shift(top, -1)
    far_top, far_low = shift(left_top, 1), shift(right_low, -1)
    acc, peak, last = near_chunks(
        (top, bottom, left_top, left_low, right_top, right_low), table
    )
    hidden, peak = call(
        far_kernel,
        None,
        tuple(local(a) for a in (far_top, far_low, last, acc, peak)),
        [shaped((kept, units), BF), shaped((8, LANES), F32)],
        (pltpu.VMEM((kept, chunk), BF),),
    )
    down = call(
        pair_kernel,
        order,
        (local(stacked), local(stacked_other)),
        shaped((chips * units, chunk), BF),
    )
    gathered = lax.all_gather(hidden, "chip", axis=0)
    outputs, peak = call(
        down_kernel,
        None,
        tuple(local(a) for a in (gathered, down, peak)),
        [shaped((X * CORES, kept // X, width), BF), shaped((8, LANES), F32)],
        (pltpu.VMEM((kept, chips * units), BF),),
    )
    returned = lax.all_to_all(outputs, ("x", "core"), split_axis=0, concat_axis=0, tiled=True)
    column = jnp.maximum(peak, partner(peak))[:2, :1]
    sums = call(
        combine_kernel,
        None,
        tuple(local(a) for a in (high, low, returned)),
        shaped((planes, rows, width), BF),
    )
    parts = lax.all_to_all(sums, "z", split_axis=0, concat_axis=0, tiled=True)
    moe_out = call(total_kernel, None, (local(parts),), shaped((rows, width), BF))
    return moe_out, column


def solution(mesh):
    devices = np.asarray(mesh.devices)
    ep, tp = devices.shape
    fine = Mesh(
        devices.reshape(X, ep // X, tp // CORES, CORES), ("x", "z", "chip", "core")
    )
    ep, tp = ("x", "z"), ("chip", "core")
    return jax.shard_map(
        layer,
        mesh=fine,
        in_specs=(
            P(ep, tp),
            P(ep, None),
            P(ep, None),
            P(ep, tp, None),
            P(ep, tp, None),
            P(ep, tp, None),
        ),
        out_specs=(P(ep, tp), P(None, ep)),
        check_vma=False,
    )
```

```python
import jax
import jax.numpy as jnp
import numpy as np
from jax import lax
from jax.experimental import pallas as pl
from jax.experimental.pallas import tpu as pltpu
from jax.sharding import Mesh, PartitionSpec as P


TOP = 8
SLOTS = 8
CORES = 2
X = 4
LANES = 128
BF = jnp.bfloat16
F32 = jnp.float32


IN_VMEM = pl.BlockSpec(memory_space=pltpu.VMEM)
IN_PLACE = pl.BlockSpec(memory_space=pltpu.HBM)
IN_SMEM = pl.BlockSpec(memory_space=pltpu.SMEM)
ROOM = pltpu.CompilerParams(vmem_limit_bytes=24 << 20)


def local(array):
    return pltpu.with_memory_space_constraint(array, pltpu.VMEM)


def remote(array):
    return pltpu.with_memory_space_constraint(array, pltpu.HBM)


def dot_nt(a, b):
    return lax.dot_general(a, b, (((1,), (1,)), ((), ())), preferred_element_type=F32)


def dot_nn(a, b):
    return lax.dot_general(a, b, (((1,), (0,)), ((), ())), preferred_element_type=F32)


def iota(shape, axis):
    return lax.broadcasted_iota(jnp.int32, shape, axis)


def run_copies(copies):
    for copy in copies:
        copy.start()
    for copy in copies:
        copy.wait()


def move(kernel, order, inputs, out_shape, count):
    single = isinstance(out_shape, jax.ShapeDtypeStruct)
    return pl.pallas_call(
        kernel,
        in_specs=[IN_SMEM] + [IN_PLACE] * len(inputs),
        out_specs=IN_PLACE if single else [IN_PLACE] * len(out_shape),
        out_shape=out_shape,
        scratch_shapes=[pltpu.SemaphoreType.DMA((count,))],
        compiler_params=ROOM,
    )(order, *(remote(array) for array in inputs))


def call(kernel, order, inputs, out_shape, scratch=(), cost=None):
    single = isinstance(out_shape, jax.ShapeDtypeStruct)
    specs = ([] if order is None else [IN_SMEM]) + [IN_VMEM] * len(inputs)
    run = pl.pallas_call(
        kernel,
        in_specs=specs,
        out_specs=IN_VMEM if single else [IN_VMEM] * len(out_shape),
        out_shape=out_shape,
        scratch_shapes=list(scratch),
        compiler_params=ROOM,
        cost_estimate=cost,
    )
    return run(*(() if order is None else (order,)), *inputs)


def pack_kernel(ids_hbm, route_hbm, tok_hbm, out_ref, ids_ref, route_ref, tok_ref, sems):
    copies = [
        pltpu.make_async_copy(source, target, sems.at[number])
        for number, (source, target) in enumerate(
            ((ids_hbm, ids_ref), (route_hbm, route_ref), (tok_hbm, tok_ref))
        )
    ]
    run_copies(copies)
    planes, height, _ = out_ref.shape
    rows, width = tok_ref.shape
    for group in range(width // LANES):
        piece = tok_ref[:, group * LANES : (group + 1) * LANES]
        for plane in range(planes):
            out_ref[plane, pl.ds(group * rows, rows), :] = piece
    lines = planes * 2 * X
    line = iota((lines, rows), 0)
    expert = (line % X) * planes + line // (2 * X)
    scale = jnp.zeros((lines, rows), F32)
    for k in range(TOP):
        scale = jnp.where(ids_ref[k : k + 1, :] == expert, route_ref[k : k + 1, :], scale)
    high = scale.astype(BF).astype(F32)
    value = jnp.where((line // X) % 2 == 0, high, scale - high).astype(BF)
    spread = (iota((rows, LANES), 1) == iota((rows, LANES), 0)).astype(F32).astype(BF)
    info = dot_nn(value, spread).reshape(planes, 2 * X, LANES)
    out_ref[:, pl.ds(height - 2 * X, 2 * X), :] = info.astype(BF)


def pack_tokens(ids, route, tokens, planes):
    rows, width = tokens.shape
    height = width // LANES * rows + 2 * X
    return pl.pallas_call(
        pack_kernel,
        in_specs=[IN_PLACE] * 3,
        out_specs=IN_VMEM,
        out_shape=jax.ShapeDtypeStruct((planes, height, LANES), BF),
        scratch_shapes=[
            pltpu.VMEM(ids.shape, ids.dtype),
            pltpu.VMEM(route.shape, route.dtype),
            pltpu.VMEM(tokens.shape, tokens.dtype),
            pltpu.SemaphoreType.DMA((3,)),
        ],
        compiler_params=ROOM,
        name="pack_tokens",
    )(remote(ids), remote(route), remote(tokens))


def route_tables(got_ref, rows):
    planes, height, _ = got_ref.shape
    span = LANES // rows
    parts = []
    for start in range(0, planes, span):
        total = None
        for plane in range(start, start + span):
            part = got_ref[plane, pl.ds(height - 2 * X, 2 * X), :].astype(F32)
            if plane > start:
                part = pltpu.roll(part, (plane - start) * rows, 1)
            total = part if total is None else total + part
        parts.append(total)
    table = jnp.concatenate(parts, axis=1)
    tokens = planes * rows
    left, right = iota((tokens, tokens), 0), iota((tokens, tokens), 1)
    before = ((left // rows == right // rows) & (left < right)).astype(F32).astype(BF)
    rank = dot_nn((table > 0.0).astype(F32).astype(BF), before)
    return table, rank


def taken_rows(table, rank, j, rows):
    tokens = table.shape[1]
    count = tokens // rows * SLOTS
    row, token = iota((count, tokens), 0), iota((count, tokens), 1)
    return (
        (table[j : j + 1, :] > 0.0)
        & (row // SLOTS == token // rows)
        & (rank[j : j + 1, :] == (row % SLOTS).astype(F32))
    )


def pick_kernel(got_ref, out_ref, tok_ref, pick_ref):
    planes, height, _ = got_ref.shape
    groups = tok_ref.shape[1] // LANES
    rows = (height - 2 * X) // groups
    table, rank = route_tables(got_ref, rows)
    for plane in range(planes):
        for group in range(groups):
            tok_ref[pl.ds(plane * rows, rows), group * LANES : (group + 1) * LANES] = got_ref[
                plane, pl.ds(group * rows, rows), :
            ]
    count = planes * SLOTS
    for j in range(X):
        pick_ref[pl.ds(j * count, count), :] = (
            taken_rows(table, rank, j, rows).astype(F32).astype(BF)
        )
    out_ref[...] = dot_nn(pick_ref[...], tok_ref[...]).astype(BF).reshape(out_ref.shape)


def weigh_kernel(got_ref, high_ref, low_ref):
    planes = got_ref.shape[0]
    rows = high_ref.shape[0] // planes
    table, rank = route_tables(got_ref, rows)
    count = planes * SLOTS
    for j in range(X):
        taken = taken_rows(table, rank, j, rows)
        for ref, line in ((high_ref, j), (low_ref, X + j)):
            value = jnp.where(taken, table[line : line + 1, :], 0.0)
            ref[:, j * count : (j + 1) * count] = value.T.astype(BF)


def join_kernel(got_ref, top_ref, low_ref):
    _, rows, width = got_ref.shape
    half = X // 2
    for x in range(X):
        ref = top_ref if x < half else low_ref
        for core in range(CORES):
            ref[pl.ds((x % half) * rows, rows), core * width : (core + 1) * width] = got_ref[
                x * CORES + core
            ]


def near_kernel(order_ref, *refs):
    pieces, (gate_own, gate_other, up_own, up_other, down_own, down_other) = refs[:6], refs[6:12]
    acc_ref, peak_ref, last_ref, down_ref, x_ref, w_ref, sems = refs[12:]
    core = order_ref[4]
    half, width = pieces[0].shape
    unit = gate_own.shape[0]
    chips = down_own.shape[0]
    own = pl.multiple_of(core * unit, unit)
    other = pl.multiple_of((1 - core) * unit, unit)
    fetched = []
    for number in range(chips):
        lanes = pl.ds(pl.multiple_of(order_ref[number] * width, width), width)
        target = w_ref.at[number] if number < 3 else last_ref
        group = []
        for place, (source, first) in enumerate(
            (
                (gate_own, own),
                (gate_other, other),
                (up_own, own + CORES * unit),
                (up_other, other + CORES * unit),
            )
        ):
            group.append(
                pltpu.make_async_copy(
                    source.at[:, lanes], target.at[pl.ds(first, unit), :], sems.at[number, place]
                )
            )
        fetched.append(group)
    handed = []
    for chip in range(chips):
        for place, (source, first) in enumerate(((down_own, own), (down_other, other))):
            rows = pl.ds(pl.multiple_of(chip * CORES * unit + first, unit), unit)
            handed.append(
                pltpu.make_async_copy(
                    source.at[chip], down_ref.at[rows, :], sems.at[chips + place, chip]
                )
            )
    for copy in [copy for group in fetched for copy in group] + handed:
        copy.start()
    peak = None
    total = None
    for number in range(3):
        x_ref[number, pl.ds(0, half), :] = pieces[2 * number][...]
        x_ref[number, pl.ds(half, half), :] = pieces[2 * number + 1][...]
        x = x_ref[number]
        for copy in fetched[number]:
            copy.wait()
        value = dot_nt(x, w_ref[number])
        total = value if total is None else total + value
        high = jnp.max(jnp.abs(x).astype(F32), axis=0, keepdims=True)
        peak = high if peak is None else jnp.maximum(peak, high)
    acc_ref[...] = total
    peak_ref[...] = peak
    for copy in fetched[3] + handed:
        copy.wait()


def near_chunks(order, pieces, weights, downs):
    half, width = pieces[0].shape
    chips, unit, _ = downs[0].shape
    wide = 2 * CORES * unit
    return pl.pallas_call(
        near_kernel,
        in_specs=[IN_SMEM] + [IN_VMEM] * 6 + [IN_PLACE] * 6,
        out_specs=[IN_VMEM] * 4,
        out_shape=[
            jax.ShapeDtypeStruct((2 * half, wide), F32),
            jax.ShapeDtypeStruct((1, width), F32),
            jax.ShapeDtypeStruct((wide, width), BF),
            jax.ShapeDtypeStruct((chips * CORES * unit, width), BF),
        ],
        scratch_shapes=[
            pltpu.VMEM((3, 2 * half, width), BF),
            pltpu.VMEM((3, wide, width), BF),
            pltpu.SemaphoreType.DMA((chips + 2, 4)),
        ],
        compiler_params=ROOM,
        cost_estimate=pl.CostEstimate(
            flops=12 * half * width * wide, transcendentals=0, bytes_accessed=12 * width * wide
        ),
        name="near_chunks",
    )(
        order,
        *(local(piece) for piece in pieces),
        *(remote(array) for array in weights),
        *(remote(array) for array in downs),
    )


def far_kernel(top_ref, low_ref, table_ref, acc_ref, peak_in, hid_ref, peak_ref, x_ref):
    half = top_ref.shape[0]
    units = hid_ref.shape[1]
    x_ref[pl.ds(0, half), :] = top_ref[...]
    x_ref[pl.ds(half, half), :] = low_ref[...]
    x = x_ref[...]
    value = acc_ref[...] + dot_nt(x, table_ref[...])
    gate = value[:, :units]
    hid_ref[...] = (gate / (1.0 + jnp.exp(-gate)) * value[:, units:]).astype(BF)
    peak = jnp.maximum(jnp.max(peak_in[...]), jnp.max(jnp.abs(x).astype(F32)))
    peak_ref[...] = jnp.full(peak_ref.shape, peak, F32)


def cut_kernel(order_ref, down_ref, *refs):
    outs, sems = refs[:-1], refs[-1]
    width = outs[0].shape[1]
    run_copies(
        [
            pltpu.make_async_copy(
                down_ref.at[:, pl.ds(pl.multiple_of(order_ref[number] * width, width), width)],
                out_ref,
                sems.at[number],
            )
            for number, out_ref in enumerate(outs)
        ]
    )


def stack_kernel(order_ref, *refs):
    pieces, (out_ref, sems) = refs[:-2], refs[-2:]
    run_copies(
        [
            pltpu.make_async_copy(piece, out_ref.at[order_ref[number]], sems.at[number])
            for number, piece in enumerate(pieces)
        ]
    )


def down_kernel(hid_ref, down_ref, peak_in, out_ref, peak_ref, h_ref):
    chips, _, units = hid_ref.shape
    for chip in range(chips):
        h_ref[:, chip * units : (chip + 1) * units] = hid_ref[chip]
    hidden = h_ref[...]
    value = dot_nn(hidden, down_ref[...]).astype(BF)
    _, rows, width = out_ref.shape
    for x in range(X):
        for core in range(CORES):
            out_ref[x * CORES + core] = value[
                x * rows : (x + 1) * rows, core * width : (core + 1) * width
            ]
    peak = jnp.max(jnp.abs(hidden).astype(F32))
    peak_ref[...] = jnp.where(iota(peak_ref.shape, 1) == 0, peak_in[...], peak)


def combine_kernel(high_ref, low_ref, row_ref, out_ref):
    rows = row_ref[...].reshape(high_ref.shape[1], row_ref.shape[2])
    value = dot_nn(high_ref[...], rows) + dot_nn(low_ref[...], rows)
    out_ref[...] = value.astype(BF).reshape(out_ref.shape)


def total_kernel(part_ref, out_ref):
    total = part_ref[0].astype(F32)
    for plane in range(1, part_ref.shape[0]):
        total = total + part_ref[plane].astype(F32)
    out_ref[...] = total.astype(BF)


def layer(tokens, expert_ids, route_weight, gate_weight, up_weight, down_weight):
    planes = lax.axis_size("z")
    chips = lax.axis_size("chip")
    core = lax.axis_index("core")
    place = lax.axis_index("chip")
    rows, width = tokens.shape
    unit, _ = gate_weight.shape[1:]
    chunk = CORES * width
    units = CORES * unit
    kept = X * planes * SLOTS // CORES
    shaped = jax.ShapeDtypeStruct

    def shift(array, step):
        return lax.ppermute(array, "chip", [(j, (j + step) % chips) for j in range(chips)])

    def partner(array):
        return lax.ppermute(array, "core", [(j, 1 - j) for j in range(CORES)])

    lane = jnp.arange(8, dtype=jnp.int32)
    turns = jnp.array([0, chips - 1, 1, 2, 0, 0, 0, 0], jnp.int32)
    order = jnp.where(
        lane < 4, (place + turns) % chips, jnp.where(lane == 4, core, lax.axis_index("z"))
    ).astype(jnp.int32)

    packed = pack_tokens(expert_ids.T, route_weight.T, tokens, planes)
    plane_rows = lax.all_to_all(packed, "z", split_axis=0, concat_axis=0, tiled=True)

    gate_other = partner(gate_weight[0])
    up_other = partner(up_weight[0])
    cuts = move(cut_kernel, order, (down_weight[0],), [shaped((unit, chunk), BF)] * chips, chips)
    pieces = [cuts[0], shift(cuts[2], 1), shift(cuts[1], -1), shift(cuts[3], 2)]
    sent = call(
        pick_kernel,
        None,
        (local(plane_rows),),
        shaped((X * CORES, kept // X, width), BF),
        (
            pltpu.VMEM((planes * rows, width), BF),
            pltpu.VMEM((X * planes * SLOTS, planes * rows), BF),
        ),
    )
    received = lax.all_to_all(sent, ("x", "core"), split_axis=0, concat_axis=0, tiled=True)
    stacked = move(stack_kernel, order, pieces, shaped((chips, unit, chunk), BF), chips)
    stacked_other = partner(stacked)
    high, low = call(
        weigh_kernel,
        None,
        (local(plane_rows),),
        [shaped((planes * rows, X * planes * SLOTS), BF)] * 2,
    )

    top, bottom = call(join_kernel, None, (local(received),), [shaped((kept // 2, chunk), BF)] * 2)
    left_top, right_low = shift(top, 1), shift(bottom, -1)
    left_low, right_top = shift(bottom, 1), shift(top, -1)
    far_top, far_low = shift(left_top, 1), shift(right_low, -1)
    acc, peak, last, down = near_chunks(
        order,
        (top, bottom, left_top, left_low, right_top, right_low),
        (gate_weight[0], gate_other, up_weight[0], up_other),
        (stacked, stacked_other),
    )
    hidden, peak = call(
        far_kernel,
        None,
        tuple(local(a) for a in (far_top, far_low, last, acc, peak)),
        [shaped((kept, units), BF), shaped((8, LANES), F32)],
        (pltpu.VMEM((kept, chunk), BF),),
    )
    gathered = lax.all_gather(hidden, "chip", axis=0)
    outputs, peak = call(
        down_kernel,
        None,
        tuple(local(a) for a in (gathered, down, peak)),
        [shaped((X * CORES, kept // X, width), BF), shaped((8, LANES), F32)],
        (pltpu.VMEM((kept, chips * units), BF),),
    )
    returned = lax.all_to_all(outputs, ("x", "core"), split_axis=0, concat_axis=0, tiled=True)
    column = jnp.maximum(peak, partner(peak))[:1, :2].T
    sums = call(
        combine_kernel,
        None,
        tuple(local(a) for a in (high, low, returned)),
        shaped((planes, rows, width), BF),
    )
    sums, column = lax.optimization_barrier((sums, column))
    parts = lax.all_to_all(sums, "z", split_axis=0, concat_axis=0, tiled=True)
    moe_out = call(total_kernel, None, (local(parts),), shaped((rows, width), BF))
    return moe_out, column


def solution(mesh):
    devices = np.asarray(mesh.devices)
    ep, tp = devices.shape
    fine = Mesh(
        devices.reshape(X, ep // X, tp // CORES, CORES), ("x", "z", "chip", "core")
    )
    ep, tp = ("x", "z"), ("chip", "core")
    return jax.shard_map(
        layer,
        mesh=fine,
        in_specs=(
            P(ep, tp),
            P(ep, None),
            P(ep, None),
            P(ep, tp, None),
            P(ep, tp, None),
            P(ep, tp, None),
        ),
        out_specs=(P(ep, tp), P(None, ep)),
        check_vma=False,
    )
```

```python
import jax
import jax.numpy as jnp
import numpy as np
from jax import lax
from jax.experimental import pallas as pl
from jax.experimental.pallas import tpu as pltpu
from jax.sharding import Mesh, PartitionSpec as P


TOP = 8
SLOTS = 8
CORES = 2
X = 4
NEAR = 4
LANES = 128
BF = jnp.bfloat16
F32 = jnp.float32


IN_VMEM = pl.BlockSpec(memory_space=pltpu.VMEM)
IN_PLACE = pl.BlockSpec(memory_space=pltpu.HBM)
IN_SMEM = pl.BlockSpec(memory_space=pltpu.SMEM)
ROOM = pltpu.CompilerParams(vmem_limit_bytes=24 << 20)


def local(array):
    return pltpu.with_memory_space_constraint(array, pltpu.VMEM)


def remote(array):
    return pltpu.with_memory_space_constraint(array, pltpu.HBM)


def dot_nt(a, b):
    return lax.dot_general(a, b, (((1,), (1,)), ((), ())), preferred_element_type=F32)


def dot_nn(a, b):
    return lax.dot_general(a, b, (((1,), (0,)), ((), ())), preferred_element_type=F32)


def iota(shape, axis):
    return lax.broadcasted_iota(jnp.int32, shape, axis)


def run_copies(copies):
    for copy in copies:
        copy.start()
    for copy in copies:
        copy.wait()


def move(kernel, order, inputs, out_shape, count):
    single = isinstance(out_shape, jax.ShapeDtypeStruct)
    return pl.pallas_call(
        kernel,
        in_specs=[IN_SMEM] + [IN_PLACE] * len(inputs),
        out_specs=IN_PLACE if single else [IN_PLACE] * len(out_shape),
        out_shape=out_shape,
        scratch_shapes=[pltpu.SemaphoreType.DMA((count,))],
        compiler_params=ROOM,
    )(order, *(remote(array) for array in inputs))


def call(kernel, order, inputs, out_shape, scratch=(), cost=None):
    single = isinstance(out_shape, jax.ShapeDtypeStruct)
    specs = ([] if order is None else [IN_SMEM]) + [IN_VMEM] * len(inputs)
    run = pl.pallas_call(
        kernel,
        in_specs=specs,
        out_specs=IN_VMEM if single else [IN_VMEM] * len(out_shape),
        out_shape=out_shape,
        scratch_shapes=list(scratch),
        compiler_params=ROOM,
        cost_estimate=cost,
    )
    return run(*(() if order is None else (order,)), *inputs)


def pack_kernel(ids_hbm, route_hbm, tok_hbm, out_ref, ids_ref, route_ref, tok_ref, sems):
    copies = [
        pltpu.make_async_copy(source, target, sems.at[number])
        for number, (source, target) in enumerate(
            ((ids_hbm, ids_ref), (route_hbm, route_ref), (tok_hbm, tok_ref))
        )
    ]
    run_copies(copies)
    planes, height, _ = out_ref.shape
    rows, width = tok_ref.shape
    for group in range(width // LANES):
        piece = tok_ref[:, group * LANES : (group + 1) * LANES]
        for plane in range(planes):
            out_ref[plane, pl.ds(group * rows, rows), :] = piece
    lines = planes * 2 * X
    line = iota((lines, rows), 0)
    expert = (line % X) * planes + line // (2 * X)
    scale = jnp.zeros((lines, rows), F32)
    for k in range(TOP):
        scale = jnp.where(ids_ref[k : k + 1, :] == expert, route_ref[k : k + 1, :], scale)
    high = scale.astype(BF).astype(F32)
    value = jnp.where((line // X) % 2 == 0, high, scale - high).astype(BF)
    spread = (iota((rows, LANES), 1) == iota((rows, LANES), 0)).astype(F32).astype(BF)
    info = dot_nn(value, spread).reshape(planes, 2 * X, LANES)
    out_ref[:, pl.ds(height - 2 * X, 2 * X), :] = info.astype(BF)


def pack_tokens(ids, route, tokens, planes):
    rows, width = tokens.shape
    height = width // LANES * rows + 2 * X
    return pl.pallas_call(
        pack_kernel,
        in_specs=[IN_PLACE] * 3,
        out_specs=IN_VMEM,
        out_shape=jax.ShapeDtypeStruct((planes, height, LANES), BF),
        scratch_shapes=[
            pltpu.VMEM(ids.shape, ids.dtype),
            pltpu.VMEM(route.shape, route.dtype),
            pltpu.VMEM(tokens.shape, tokens.dtype),
            pltpu.SemaphoreType.DMA((3,)),
        ],
        compiler_params=ROOM,
        name="pack_tokens",
    )(remote(ids), remote(route), remote(tokens))


def route_tables(got_ref, rows):
    planes, height, _ = got_ref.shape
    span = LANES // rows
    parts = []
    for start in range(0, planes, span):
        total = None
        for plane in range(start, start + span):
            part = got_ref[plane, pl.ds(height - 2 * X, 2 * X), :].astype(F32)
            if plane > start:
                part = pltpu.roll(part, (plane - start) * rows, 1)
            total = part if total is None else total + part
        parts.append(total)
    table = jnp.concatenate(parts, axis=1)
    tokens = planes * rows
    left, right = iota((tokens, tokens), 0), iota((tokens, tokens), 1)
    before = ((left // rows == right // rows) & (left < right)).astype(F32).astype(BF)
    rank = dot_nn((table > 0.0).astype(F32).astype(BF), before)
    return table, rank


def taken_rows(table, rank, j, rows):
    tokens = table.shape[1]
    count = tokens // rows * SLOTS
    row, token = iota((count, tokens), 0), iota((count, tokens), 1)
    return (
        (table[j : j + 1, :] > 0.0)
        & (row // SLOTS == token // rows)
        & (rank[j : j + 1, :] == (row % SLOTS).astype(F32))
    )


def pick_kernel(got_ref, out_ref, tok_ref, pick_ref):
    planes, height, _ = got_ref.shape
    groups = tok_ref.shape[1] // LANES
    rows = (height - 2 * X) // groups
    table, rank = route_tables(got_ref, rows)
    for plane in range(planes):
        for group in range(groups):
            tok_ref[pl.ds(plane * rows, rows), group * LANES : (group + 1) * LANES] = got_ref[
                plane, pl.ds(group * rows, rows), :
            ]
    count = planes * SLOTS
    for j in range(X):
        pick_ref[pl.ds(j * count, count), :] = (
            taken_rows(table, rank, j, rows).astype(F32).astype(BF)
        )
    out_ref[...] = dot_nn(pick_ref[...], tok_ref[...]).astype(BF).reshape(out_ref.shape)


def weigh_kernel(got_ref, high_ref, low_ref):
    planes = got_ref.shape[0]
    rows = high_ref.shape[0] // planes
    table, rank = route_tables(got_ref, rows)
    count = planes * SLOTS
    for j in range(X):
        taken = taken_rows(table, rank, j, rows)
        for ref, line in ((high_ref, j), (low_ref, X + j)):
            value = jnp.where(taken, table[line : line + 1, :], 0.0)
            ref[:, j * count : (j + 1) * count] = value.T.astype(BF)


def join_kernel(got_ref, top_ref, low_ref):
    _, rows, width = got_ref.shape
    half = X // 2
    for x in range(X):
        ref = top_ref if x < half else low_ref
        for core in range(CORES):
            ref[pl.ds((x % half) * rows, rows), core * width : (core + 1) * width] = got_ref[
                x * CORES + core
            ]


def near_kernel(order_ref, *refs):
    pieces, (gate_own, gate_other, up_own, up_other, down_own, down_other) = refs[:6], refs[6:12]
    acc_ref, peak_ref, last_ref, down_ref, x_ref, w_ref, sems = refs[12:]
    core = order_ref[4]
    half, width = pieces[0].shape
    unit = gate_own.shape[0]
    chips = down_own.shape[0]
    own = pl.multiple_of(core * unit, unit)
    other = pl.multiple_of((1 - core) * unit, unit)
    fetched = []
    for number in range(chips):
        lanes = pl.ds(pl.multiple_of(order_ref[number] * width, width), width)
        target = w_ref.at[number] if number < 3 else last_ref
        group = []
        for place, (source, first) in enumerate(
            (
                (gate_own, own),
                (gate_other, other),
                (up_own, own + CORES * unit),
                (up_other, other + CORES * unit),
            )
        ):
            group.append(
                pltpu.make_async_copy(
                    source.at[:, lanes], target.at[pl.ds(first, unit), :], sems.at[number, place]
                )
            )
        fetched.append(group)
    handed = []
    for chip in range(chips):
        for place, (source, first) in enumerate(((down_own, own), (down_other, other))):
            rows = pl.ds(pl.multiple_of(chip * CORES * unit + first, unit), unit)
            handed.append(
                pltpu.make_async_copy(
                    source.at[chip], down_ref.at[rows, :], sems.at[chips + place, chip]
                )
            )
    for copy in [copy for group in fetched for copy in group] + handed:
        copy.start()
    peak = None
    total = None
    for number in range(3):
        x_ref[number, pl.ds(0, half), :] = pieces[2 * number][...]
        x_ref[number, pl.ds(half, half), :] = pieces[2 * number + 1][...]
        x = x_ref[number]
        for copy in fetched[number]:
            copy.wait()
        value = dot_nt(x, w_ref[number])
        total = value if total is None else total + value
        high = jnp.max(jnp.abs(x).astype(F32), axis=0, keepdims=True)
        peak = high if peak is None else jnp.maximum(peak, high)
    acc_ref[...] = total
    peak_ref[...] = peak
    for copy in fetched[3] + handed:
        copy.wait()


def near_chunks(order, pieces, weights, downs):
    half, width = pieces[0].shape
    chips, unit, _ = downs[0].shape
    wide = 2 * CORES * unit
    return pl.pallas_call(
        near_kernel,
        in_specs=[IN_SMEM] + [IN_VMEM] * 6 + [IN_PLACE] * 6,
        out_specs=[IN_VMEM] * 4,
        out_shape=[
            jax.ShapeDtypeStruct((2 * half, wide), F32),
            jax.ShapeDtypeStruct((1, width), F32),
            jax.ShapeDtypeStruct((wide, width), BF),
            jax.ShapeDtypeStruct((chips * CORES * unit, width), BF),
        ],
        scratch_shapes=[
            pltpu.VMEM((3, 2 * half, width), BF),
            pltpu.VMEM((3, wide, width), BF),
            pltpu.SemaphoreType.DMA((chips + 2, 4)),
        ],
        compiler_params=ROOM,
        cost_estimate=pl.CostEstimate(
            flops=12 * half * width * wide, transcendentals=0, bytes_accessed=12 * width * wide
        ),
        name="near_chunks",
    )(
        order,
        *(local(piece) for piece in pieces),
        *(remote(array) for array in weights),
        *(remote(array) for array in downs),
    )


def far_kernel(top_ref, low_ref, table_ref, acc_ref, peak_in, hid_ref, peak_ref, x_ref):
    half = top_ref.shape[0]
    units = hid_ref.shape[1]
    x_ref[pl.ds(0, half), :] = top_ref[...]
    x_ref[pl.ds(half, half), :] = low_ref[...]
    x = x_ref[...]
    value = acc_ref[...] + dot_nt(x, table_ref[...])
    gate = value[:, :units]
    hid_ref[...] = (gate / (1.0 + jnp.exp(-gate)) * value[:, units:]).astype(BF)
    peak = jnp.maximum(jnp.max(peak_in[...]), jnp.max(jnp.abs(x).astype(F32)))
    peak_ref[...] = jnp.full(peak_ref.shape, peak, F32)


def cut_kernel(order_ref, down_ref, *refs):
    outs, sems = refs[:-1], refs[-1]
    width = outs[0].shape[1]
    run_copies(
        [
            pltpu.make_async_copy(
                down_ref.at[:, pl.ds(pl.multiple_of(order_ref[number] * width, width), width)],
                out_ref,
                sems.at[number],
            )
            for number, out_ref in enumerate(outs)
        ]
    )


def stack_kernel(order_ref, *refs):
    pieces, (out_ref, sems) = refs[:-2], refs[-2:]
    run_copies(
        [
            pltpu.make_async_copy(piece, out_ref.at[order_ref[number]], sems.at[number])
            for number, piece in enumerate(pieces)
        ]
    )


def down_kernel(hid_ref, down_ref, peak_in, out_ref, peak_ref, h_ref):
    chips, _, units = hid_ref.shape
    for chip in range(chips):
        h_ref[:, chip * units : (chip + 1) * units] = hid_ref[chip]
    hidden = h_ref[...]
    value = dot_nn(hidden, down_ref[...]).astype(BF)
    _, rows, width = out_ref.shape
    for x in range(X):
        for core in range(CORES):
            out_ref[x * CORES + core] = value[
                x * rows : (x + 1) * rows, core * width : (core + 1) * width
            ]
    peak = jnp.max(jnp.abs(hidden).astype(F32))
    peak_ref[...] = jnp.where(iota(peak_ref.shape, 1) == 0, peak_in[...], peak)


def combine_kernel(high_ref, low_ref, row_ref, out_ref):
    rows = row_ref[...].reshape(high_ref.shape[1], row_ref.shape[2])
    value = dot_nn(high_ref[...], rows) + dot_nn(low_ref[...], rows)
    value = value.astype(BF)
    near, blocks, rows, _ = out_ref.shape
    for low in range(near):
        for high in range(blocks):
            start = (high * near + low) * rows
            out_ref[low, high] = value[start : start + rows]


def total_kernel(part_ref, out_ref):
    total = part_ref[0].astype(F32)
    for plane in range(1, part_ref.shape[0]):
        total = total + part_ref[plane].astype(F32)
    out_ref[...] = total.astype(BF)


def layer(tokens, expert_ids, route_weight, gate_weight, up_weight, down_weight):
    near = lax.axis_size("zlow")
    planes = lax.axis_size("zhigh") * near
    chips = lax.axis_size("chip")
    core = lax.axis_index("core")
    place = lax.axis_index("chip")
    rows, width = tokens.shape
    unit, _ = gate_weight.shape[1:]
    chunk = CORES * width
    units = CORES * unit
    kept = X * planes * SLOTS // CORES
    shaped = jax.ShapeDtypeStruct

    def shift(array, step):
        return lax.ppermute(array, "chip", [(j, (j + step) % chips) for j in range(chips)])

    def partner(array):
        return lax.ppermute(array, "core", [(j, 1 - j) for j in range(CORES)])

    lane = jnp.arange(8, dtype=jnp.int32)
    turns = jnp.array([0, chips - 1, 1, 2, 0, 0, 0, 0], jnp.int32)
    order = jnp.where(
        lane < 4, (place + turns) % chips, core
    ).astype(jnp.int32)

    packed = pack_tokens(expert_ids.T, route_weight.T, tokens, planes)
    plane_rows = lax.all_to_all(packed, ("zhigh", "zlow"), split_axis=0, concat_axis=0, tiled=True)

    gate_other = partner(gate_weight[0])
    up_other = partner(up_weight[0])
    cuts = move(cut_kernel, order, (down_weight[0],), [shaped((unit, chunk), BF)] * chips, chips)
    pieces = [cuts[0], shift(cuts[2], 1), shift(cuts[1], -1), shift(cuts[3], 2)]
    sent = call(
        pick_kernel,
        None,
        (local(plane_rows),),
        shaped((X * CORES, kept // X, width), BF),
        (
            pltpu.VMEM((planes * rows, width), BF),
            pltpu.VMEM((X * planes * SLOTS, planes * rows), BF),
        ),
    )
    received = lax.all_to_all(sent, ("x", "core"), split_axis=0, concat_axis=0, tiled=True)
    stacked = move(stack_kernel, order, pieces, shaped((chips, unit, chunk), BF), chips)
    stacked_other = partner(stacked)
    high, low = call(
        weigh_kernel,
        None,
        (local(plane_rows),),
        [shaped((planes * rows, X * planes * SLOTS), BF)] * 2,
    )

    top, bottom = call(join_kernel, None, (local(received),), [shaped((kept // 2, chunk), BF)] * 2)
    left_top, right_low = shift(top, 1), shift(bottom, -1)
    left_low, right_top = shift(bottom, 1), shift(top, -1)
    far_top, far_low = shift(left_top, 1), shift(right_low, -1)
    acc, peak, last, down = near_chunks(
        order,
        (top, bottom, left_top, left_low, right_top, right_low),
        (gate_weight[0], gate_other, up_weight[0], up_other),
        (stacked, stacked_other),
    )
    hidden, peak = call(
        far_kernel,
        None,
        tuple(local(a) for a in (far_top, far_low, last, acc, peak)),
        [shaped((kept, units), BF), shaped((8, LANES), F32)],
        (pltpu.VMEM((kept, chunk), BF),),
    )
    gathered = lax.all_gather(hidden, "chip", axis=0)
    outputs, peak = call(
        down_kernel,
        None,
        tuple(local(a) for a in (gathered, down, peak)),
        [shaped((X * CORES, kept // X, width), BF), shaped((8, LANES), F32)],
        (pltpu.VMEM((kept, chips * units), BF),),
    )
    returned = lax.all_to_all(outputs, ("x", "core"), split_axis=0, concat_axis=0, tiled=True)
    column = jnp.maximum(peak, partner(peak))[:1, :2].T
    sums = call(
        combine_kernel,
        None,
        tuple(local(a) for a in (high, low, returned)),
        shaped((near, planes // near, rows, width), BF),
    )
    sums, column = lax.optimization_barrier((sums, column))
    parts = lax.all_to_all(sums, "zlow", split_axis=0, concat_axis=0, tiled=True)
    sums = call(total_kernel, None, (local(parts),), shaped((planes // near, rows, width), BF))
    parts = lax.all_to_all(sums, "zhigh", split_axis=0, concat_axis=0, tiled=True)
    moe_out = call(total_kernel, None, (local(parts),), shaped((rows, width), BF))
    return moe_out, column


def solution(mesh):
    devices = np.asarray(mesh.devices)
    ep, tp = devices.shape
    fine = Mesh(
        devices.reshape(X, ep // (X * NEAR), NEAR, tp // CORES, CORES),
        ("x", "zhigh", "zlow", "chip", "core"),
    )
    ep, tp = ("x", "zhigh", "zlow"), ("chip", "core")
    return jax.shard_map(
        layer,
        mesh=fine,
        in_specs=(
            P(ep, tp),
            P(ep, None),
            P(ep, None),
            P(ep, tp, None),
            P(ep, tp, None),
            P(ep, tp, None),
        ),
        out_specs=(P(ep, tp), P(None, ep)),
        check_vma=False,
    )
```

```python
import jax
import jax.numpy as jnp
import numpy as np
from jax import lax
from jax.experimental import pallas as pl
from jax.experimental.pallas import tpu as pltpu
from jax.sharding import Mesh, PartitionSpec as P


TOP = 8
SLOTS = 8
CORES = 2
X = 4
LANES = 128
BF = jnp.bfloat16
F32 = jnp.float32


IN_VMEM = pl.BlockSpec(memory_space=pltpu.VMEM)
IN_PLACE = pl.BlockSpec(memory_space=pltpu.HBM)
IN_SMEM = pl.BlockSpec(memory_space=pltpu.SMEM)
ROOM = pltpu.CompilerParams(vmem_limit_bytes=24 << 20)


def local(array):
    return pltpu.with_memory_space_constraint(array, pltpu.VMEM)


def remote(array):
    return pltpu.with_memory_space_constraint(array, pltpu.HBM)


def dot_nt(a, b):
    return lax.dot_general(a, b, (((1,), (1,)), ((), ())), preferred_element_type=F32)


def dot_nn(a, b):
    return lax.dot_general(a, b, (((1,), (0,)), ((), ())), preferred_element_type=F32)


def iota(shape, axis):
    return lax.broadcasted_iota(jnp.int32, shape, axis)


def run_copies(copies):
    for copy in copies:
        copy.start()
    for copy in copies:
        copy.wait()


def move(kernel, order, inputs, out_shape, count):
    single = isinstance(out_shape, jax.ShapeDtypeStruct)
    return pl.pallas_call(
        kernel,
        in_specs=[IN_SMEM] + [IN_PLACE] * len(inputs),
        out_specs=IN_PLACE if single else [IN_PLACE] * len(out_shape),
        out_shape=out_shape,
        scratch_shapes=[pltpu.SemaphoreType.DMA((count,))],
        compiler_params=ROOM,
    )(order, *(remote(array) for array in inputs))


def call(kernel, order, inputs, out_shape, scratch=(), cost=None):
    single = isinstance(out_shape, jax.ShapeDtypeStruct)
    specs = ([] if order is None else [IN_SMEM]) + [IN_VMEM] * len(inputs)
    run = pl.pallas_call(
        kernel,
        in_specs=specs,
        out_specs=IN_VMEM if single else [IN_VMEM] * len(out_shape),
        out_shape=out_shape,
        scratch_shapes=list(scratch),
        compiler_params=ROOM,
        cost_estimate=cost,
    )
    return run(*(() if order is None else (order,)), *inputs)


def pack_kernel(ids_hbm, route_hbm, tok_hbm, out_ref, ids_ref, route_ref, tok_ref, sems):
    copies = [
        pltpu.make_async_copy(source, target, sems.at[number])
        for number, (source, target) in enumerate(
            ((ids_hbm, ids_ref), (route_hbm, route_ref), (tok_hbm, tok_ref))
        )
    ]
    run_copies(copies)
    planes, height, _ = out_ref.shape
    rows, width = tok_ref.shape
    for group in range(width // LANES):
        piece = tok_ref[:, group * LANES : (group + 1) * LANES]
        for plane in range(planes):
            out_ref[plane, pl.ds(group * rows, rows), :] = piece
    lines = planes * 2 * X
    line = iota((lines, rows), 0)
    expert = (line % X) * planes + line // (2 * X)
    scale = jnp.zeros((lines, rows), F32)
    for k in range(TOP):
        scale = jnp.where(ids_ref[k : k + 1, :] == expert, route_ref[k : k + 1, :], scale)
    high = scale.astype(BF).astype(F32)
    value = jnp.where((line // X) % 2 == 0, high, scale - high).astype(BF)
    spread = (iota((rows, LANES), 1) == iota((rows, LANES), 0)).astype(F32).astype(BF)
    info = dot_nn(value, spread).reshape(planes, 2 * X, LANES)
    out_ref[:, pl.ds(height - 2 * X, 2 * X), :] = info.astype(BF)


def pack_tokens(ids, route, tokens, planes):
    rows, width = tokens.shape
    height = width // LANES * rows + 2 * X
    return pl.pallas_call(
        pack_kernel,
        in_specs=[IN_PLACE] * 3,
        out_specs=IN_VMEM,
        out_shape=jax.ShapeDtypeStruct((planes, height, LANES), BF),
        scratch_shapes=[
            pltpu.VMEM(ids.shape, ids.dtype),
            pltpu.VMEM(route.shape, route.dtype),
            pltpu.VMEM(tokens.shape, tokens.dtype),
            pltpu.SemaphoreType.DMA((3,)),
        ],
        compiler_params=ROOM,
        name="pack_tokens",
    )(remote(ids), remote(route), remote(tokens))


def route_tables(got_ref, rows):
    planes, height, _ = got_ref.shape
    span = LANES // rows
    parts = []
    for start in range(0, planes, span):
        total = None
        for plane in range(start, start + span):
            part = got_ref[plane, pl.ds(height - 2 * X, 2 * X), :].astype(F32)
            if plane > start:
                part = pltpu.roll(part, (plane - start) * rows, 1)
            total = part if total is None else total + part
        parts.append(total)
    table = jnp.concatenate(parts, axis=1)
    tokens = planes * rows
    left, right = iota((tokens, tokens), 0), iota((tokens, tokens), 1)
    before = ((left // rows == right // rows) & (left < right)).astype(F32).astype(BF)
    rank = dot_nn((table > 0.0).astype(F32).astype(BF), before)
    return table, rank


def taken_rows(table, rank, j, rows):
    tokens = table.shape[1]
    count = tokens // rows * SLOTS
    row, token = iota((count, tokens), 0), iota((count, tokens), 1)
    return (
        (table[j : j + 1, :] > 0.0)
        & (row // SLOTS == token // rows)
        & (rank[j : j + 1, :] == (row % SLOTS).astype(F32))
    )


def pick_kernel(got_ref, out_ref, tok_ref, pick_ref):
    planes, height, _ = got_ref.shape
    groups = tok_ref.shape[1] // LANES
    rows = (height - 2 * X) // groups
    table, rank = route_tables(got_ref, rows)
    for plane in range(planes):
        for group in range(groups):
            tok_ref[pl.ds(plane * rows, rows), group * LANES : (group + 1) * LANES] = got_ref[
                plane, pl.ds(group * rows, rows), :
            ]
    count = planes * SLOTS
    for j in range(X):
        pick_ref[pl.ds(j * count, count), :] = (
            taken_rows(table, rank, j, rows).astype(F32).astype(BF)
        )
    out_ref[...] = dot_nn(pick_ref[...], tok_ref[...]).astype(BF).reshape(out_ref.shape)


def weigh_kernel(got_ref, high_ref, low_ref):
    planes = got_ref.shape[0]
    rows = high_ref.shape[0] // planes
    table, rank = route_tables(got_ref, rows)
    count = planes * SLOTS
    for j in range(X):
        taken = taken_rows(table, rank, j, rows)
        for ref, line in ((high_ref, j), (low_ref, X + j)):
            value = jnp.where(taken, table[line : line + 1, :], 0.0)
            ref[:, j * count : (j + 1) * count] = value.T.astype(BF)


def join_kernel(got_ref, top_ref, low_ref):
    _, rows, width = got_ref.shape
    half = X // 2
    for x in range(X):
        ref = top_ref if x < half else low_ref
        for core in range(CORES):
            ref[pl.ds((x % half) * rows, rows), core * width : (core + 1) * width] = got_ref[
                x * CORES + core
            ]


def near_kernel(order_ref, *refs):
    pieces, (gate_own, gate_other, up_own, up_other, down_own, down_other) = refs[:6], refs[6:12]
    acc_ref, peak_ref, last_ref, down_ref, x_ref, w_ref, sems = refs[12:]
    core = order_ref[4]
    half, width = pieces[0].shape
    unit = gate_own.shape[0]
    chips = down_own.shape[0]
    own = pl.multiple_of(core * unit, unit)
    other = pl.multiple_of((1 - core) * unit, unit)
    fetched = []
    for number in range(chips):
        lanes = pl.ds(pl.multiple_of(order_ref[number] * width, width), width)
        target = w_ref.at[number] if number < 3 else last_ref
        group = []
        for place, (source, first) in enumerate(
            (
                (gate_own, own),
                (gate_other, other),
                (up_own, own + CORES * unit),
                (up_other, other + CORES * unit),
            )
        ):
            group.append(
                pltpu.make_async_copy(
                    source.at[:, lanes], target.at[pl.ds(first, unit), :], sems.at[number, place]
                )
            )
        fetched.append(group)
    handed = []
    for chip in range(chips):
        for place, (source, first) in enumerate(((down_own, own), (down_other, other))):
            rows = pl.ds(pl.multiple_of(chip * CORES * unit + first, unit), unit)
            handed.append(
                pltpu.make_async_copy(
                    source.at[chip], down_ref.at[rows, :], sems.at[chips + place, chip]
                )
            )
    stages = fetched + [handed]
    for copy in stages[0] + stages[1]:
        copy.start()
    peak = None
    total = None
    for number in range(3):
        x_ref[number, pl.ds(0, half), :] = pieces[2 * number][...]
        x_ref[number, pl.ds(half, half), :] = pieces[2 * number + 1][...]
        x = x_ref[number]
        for copy in stages[number]:
            copy.wait()
        for copy in stages[number + 2]:
            copy.start()
        value = dot_nt(x, w_ref[number])
        total = value if total is None else total + value
        high = jnp.max(jnp.abs(x).astype(F32), axis=0, keepdims=True)
        peak = high if peak is None else jnp.maximum(peak, high)
    acc_ref[...] = total
    peak_ref[...] = peak
    for copy in stages[3] + stages[4]:
        copy.wait()


def near_chunks(order, pieces, weights, downs):
    half, width = pieces[0].shape
    chips, unit, _ = downs[0].shape
    wide = 2 * CORES * unit
    return pl.pallas_call(
        near_kernel,
        in_specs=[IN_SMEM] + [IN_VMEM] * 6 + [IN_PLACE] * 6,
        out_specs=[IN_VMEM] * 4,
        out_shape=[
            jax.ShapeDtypeStruct((2 * half, wide), F32),
            jax.ShapeDtypeStruct((1, width), F32),
            jax.ShapeDtypeStruct((wide, width), BF),
            jax.ShapeDtypeStruct((chips * CORES * unit, width), BF),
        ],
        scratch_shapes=[
            pltpu.VMEM((3, 2 * half, width), BF),
            pltpu.VMEM((3, wide, width), BF),
            pltpu.SemaphoreType.DMA((chips + 2, 4)),
        ],
        compiler_params=ROOM,
        cost_estimate=pl.CostEstimate(
            flops=12 * half * width * wide, transcendentals=0, bytes_accessed=12 * width * wide
        ),
        name="near_chunks",
    )(
        order,
        *(local(piece) for piece in pieces),
        *(remote(array) for array in weights),
        *(remote(array) for array in downs),
    )


def far_kernel(top_ref, low_ref, table_ref, acc_ref, peak_in, hid_ref, peak_ref, x_ref):
    half = top_ref.shape[0]
    units = hid_ref.shape[1]
    x_ref[pl.ds(0, half), :] = top_ref[...]
    x_ref[pl.ds(half, half), :] = low_ref[...]
    x = x_ref[...]
    value = acc_ref[...] + dot_nt(x, table_ref[...])
    gate = value[:, :units]
    hid_ref[...] = (gate / (1.0 + jnp.exp(-gate)) * value[:, units:]).astype(BF)
    peak = jnp.maximum(jnp.max(peak_in[...]), jnp.max(jnp.abs(x).astype(F32)))
    peak_ref[...] = jnp.full(peak_ref.shape, peak, F32)


def cut_kernel(order_ref, down_ref, *refs):
    outs, sems = refs[:-1], refs[-1]
    width = outs[0].shape[1]
    run_copies(
        [
            pltpu.make_async_copy(
                down_ref.at[:, pl.ds(pl.multiple_of(order_ref[number] * width, width), width)],
                out_ref,
                sems.at[number],
            )
            for number, out_ref in enumerate(outs)
        ]
    )


def stack_kernel(order_ref, *refs):
    pieces, (out_ref, sems) = refs[:-2], refs[-2:]
    run_copies(
        [
            pltpu.make_async_copy(piece, out_ref.at[order_ref[number]], sems.at[number])
            for number, piece in enumerate(pieces)
        ]
    )


def down_kernel(hid_ref, down_ref, peak_in, out_ref, peak_ref, h_ref):
    chips, _, units = hid_ref.shape
    for chip in range(chips):
        h_ref[:, chip * units : (chip + 1) * units] = hid_ref[chip]
    hidden = h_ref[...]
    value = dot_nn(hidden, down_ref[...]).astype(BF)
    _, rows, width = out_ref.shape
    for x in range(X):
        for core in range(CORES):
            out_ref[x * CORES + core] = value[
                x * rows : (x + 1) * rows, core * width : (core + 1) * width
            ]
    peak = jnp.max(jnp.abs(hidden).astype(F32))
    peak_ref[...] = jnp.where(iota(peak_ref.shape, 1) == 0, peak_in[...], peak)


def combine_kernel(high_ref, low_ref, row_ref, out_ref):
    rows = row_ref[...].reshape(high_ref.shape[1], row_ref.shape[2])
    value = dot_nn(high_ref[...], rows) + dot_nn(low_ref[...], rows)
    out_ref[...] = value.astype(BF).reshape(out_ref.shape)


def total_kernel(part_ref, out_ref):
    total = part_ref[0].astype(F32)
    for plane in range(1, part_ref.shape[0]):
        total = total + part_ref[plane].astype(F32)
    out_ref[...] = total.astype(BF)


def layer(tokens, expert_ids, route_weight, gate_weight, up_weight, down_weight):
    planes = lax.axis_size("z")
    chips = lax.axis_size("chip")
    core = lax.axis_index("core")
    place = lax.axis_index("chip")
    rows, width = tokens.shape
    unit, _ = gate_weight.shape[1:]
    chunk = CORES * width
    units = CORES * unit
    kept = X * planes * SLOTS // CORES
    shaped = jax.ShapeDtypeStruct

    def swap(array, mask):
        return lax.ppermute(array, "chip", [(j, j ^ mask) for j in range(chips)])

    def partner(array):
        return lax.ppermute(array, "core", [(j, 1 - j) for j in range(CORES)])

    lane = jnp.arange(8, dtype=jnp.int32)
    order = jnp.where(
        lane < 2, place ^ lane, jnp.where(lane < 4, place ^ (5 - lane), core)
    ).astype(jnp.int32)

    packed = pack_tokens(expert_ids.T, route_weight.T, tokens, planes)
    plane_rows = lax.all_to_all(packed, "z", split_axis=0, concat_axis=0, tiled=True)

    gate_other = partner(gate_weight[0])
    up_other = partner(up_weight[0])
    cuts = move(cut_kernel, order, (down_weight[0],), [shaped((unit, chunk), BF)] * chips, chips)
    pieces = [cuts[0], swap(cuts[1], 1), swap(cuts[2], 3), swap(cuts[3], 2)]
    sent = call(
        pick_kernel,
        None,
        (local(plane_rows),),
        shaped((X * CORES, kept // X, width), BF),
        (
            pltpu.VMEM((planes * rows, width), BF),
            pltpu.VMEM((X * planes * SLOTS, planes * rows), BF),
        ),
    )
    received = lax.all_to_all(sent, ("x", "core"), split_axis=0, concat_axis=0, tiled=True)
    stacked = move(stack_kernel, order, pieces, shaped((chips, unit, chunk), BF), chips)
    stacked_other = partner(stacked)
    high, low = call(
        weigh_kernel,
        None,
        (local(plane_rows),),
        [shaped((planes * rows, X * planes * SLOTS), BF)] * 2,
    )

    top, bottom = call(join_kernel, None, (local(received),), [shaped((kept // 2, chunk), BF)] * 2)
    cross_top = swap(top, 3)
    beside_low = swap(bottom, 1)
    cross_low = swap(bottom, 3)
    beside_top = swap(top, 1)
    far_top, far_low = swap(cross_top, 1), swap(beside_low, 3)
    acc, peak, last, down = near_chunks(
        order,
        (top, bottom, beside_top, beside_low, cross_top, cross_low),
        (gate_weight[0], gate_other, up_weight[0], up_other),
        (stacked, stacked_other),
    )
    hidden, peak = call(
        far_kernel,
        None,
        tuple(local(a) for a in (far_top, far_low, last, acc, peak)),
        [shaped((kept, units), BF), shaped((8, LANES), F32)],
        (pltpu.VMEM((kept, chunk), BF),),
    )
    gathered = lax.all_gather(hidden, "chip", axis=0)
    outputs, peak = call(
        down_kernel,
        None,
        tuple(local(a) for a in (gathered, down, peak)),
        [shaped((X * CORES, kept // X, width), BF), shaped((8, LANES), F32)],
        (pltpu.VMEM((kept, chips * units), BF),),
    )
    returned = lax.all_to_all(outputs, ("x", "core"), split_axis=0, concat_axis=0, tiled=True)
    column = jnp.maximum(peak, partner(peak))[:1, :2].T
    sums = call(
        combine_kernel,
        None,
        tuple(local(a) for a in (high, low, returned)),
        shaped((planes, rows, width), BF),
    )
    sums, column = lax.optimization_barrier((sums, column))
    parts = lax.all_to_all(sums, "z", split_axis=0, concat_axis=0, tiled=True)
    moe_out = call(total_kernel, None, (local(parts),), shaped((rows, width), BF))
    return moe_out, column


def solution(mesh):
    devices = np.asarray(mesh.devices)
    ep, tp = devices.shape
    fine = Mesh(
        devices.reshape(X, ep // X, tp // CORES, CORES), ("x", "z", "chip", "core")
    )
    ep, tp = ("x", "z"), ("chip", "core")
    return jax.shard_map(
        layer,
        mesh=fine,
        in_specs=(
            P(ep, tp),
            P(ep, None),
            P(ep, None),
            P(ep, tp, None),
            P(ep, tp, None),
            P(ep, tp, None),
        ),
        out_specs=(P(ep, tp), P(None, ep)),
        check_vma=False,
    )
```

```python
import jax
import jax.numpy as jnp
import numpy as np
from jax import lax
from jax.experimental import pallas as pl
from jax.experimental.pallas import tpu as pltpu
from jax.sharding import Mesh, PartitionSpec as P


TOP = 8
SLOTS = 8
CORES = 2
X = 4
LANES = 128
BF = jnp.bfloat16
F32 = jnp.float32


IN_VMEM = pl.BlockSpec(memory_space=pltpu.VMEM)
IN_PLACE = pl.BlockSpec(memory_space=pltpu.HBM)
IN_SMEM = pl.BlockSpec(memory_space=pltpu.SMEM)
ROOM = pltpu.CompilerParams(vmem_limit_bytes=24 << 20)


def local(array):
    return pltpu.with_memory_space_constraint(array, pltpu.VMEM)


def remote(array):
    return pltpu.with_memory_space_constraint(array, pltpu.HBM)


def dot_nt(a, b):
    return lax.dot_general(a, b, (((1,), (1,)), ((), ())), preferred_element_type=F32)


def dot_nn(a, b):
    return lax.dot_general(a, b, (((1,), (0,)), ((), ())), preferred_element_type=F32)


def iota(shape, axis):
    return lax.broadcasted_iota(jnp.int32, shape, axis)


def run_copies(copies):
    for copy in copies:
        copy.start()
    for copy in copies:
        copy.wait()


def move(kernel, order, inputs, out_shape, count):
    single = isinstance(out_shape, jax.ShapeDtypeStruct)
    return pl.pallas_call(
        kernel,
        in_specs=[IN_SMEM] + [IN_PLACE] * len(inputs),
        out_specs=IN_PLACE if single else [IN_PLACE] * len(out_shape),
        out_shape=out_shape,
        scratch_shapes=[pltpu.SemaphoreType.DMA((count,))],
        compiler_params=ROOM,
    )(order, *(remote(array) for array in inputs))


def call(kernel, order, inputs, out_shape, scratch=(), cost=None):
    single = isinstance(out_shape, jax.ShapeDtypeStruct)
    specs = ([] if order is None else [IN_SMEM]) + [IN_VMEM] * len(inputs)
    run = pl.pallas_call(
        kernel,
        in_specs=specs,
        out_specs=IN_VMEM if single else [IN_VMEM] * len(out_shape),
        out_shape=out_shape,
        scratch_shapes=list(scratch),
        compiler_params=ROOM,
        cost_estimate=cost,
    )
    return run(*(() if order is None else (order,)), *inputs)


def pack_kernel(ids_hbm, route_hbm, tok_hbm, out_ref, ids_ref, route_ref, tok_ref, sems):
    copies = [
        pltpu.make_async_copy(source, target, sems.at[number])
        for number, (source, target) in enumerate(
            ((ids_hbm, ids_ref), (route_hbm, route_ref), (tok_hbm, tok_ref))
        )
    ]
    run_copies(copies)
    planes, height, _ = out_ref.shape
    rows, width = tok_ref.shape
    for group in range(width // LANES):
        piece = tok_ref[:, group * LANES : (group + 1) * LANES]
        for plane in range(planes):
            out_ref[plane, pl.ds(group * rows, rows), :] = piece
    lines = planes * 2 * X
    line = iota((lines, rows), 0)
    expert = (line % X) * planes + line // (2 * X)
    scale = jnp.zeros((lines, rows), F32)
    for k in range(TOP):
        scale = jnp.where(ids_ref[k : k + 1, :] == expert, route_ref[k : k + 1, :], scale)
    high = scale.astype(BF).astype(F32)
    value = jnp.where((line // X) % 2 == 0, high, scale - high).astype(BF)
    spread = (iota((rows, LANES), 1) == iota((rows, LANES), 0)).astype(F32).astype(BF)
    info = dot_nn(value, spread).reshape(planes, 2 * X, LANES)
    out_ref[:, pl.ds(height - 2 * X, 2 * X), :] = info.astype(BF)


def pack_tokens(ids, route, tokens, planes):
    rows, width = tokens.shape
    height = width // LANES * rows + 2 * X
    return pl.pallas_call(
        pack_kernel,
        in_specs=[IN_PLACE] * 3,
        out_specs=IN_VMEM,
        out_shape=jax.ShapeDtypeStruct((planes, height, LANES), BF),
        scratch_shapes=[
            pltpu.VMEM(ids.shape, ids.dtype),
            pltpu.VMEM(route.shape, route.dtype),
            pltpu.VMEM(tokens.shape, tokens.dtype),
            pltpu.SemaphoreType.DMA((3,)),
        ],
        compiler_params=ROOM,
        name="pack_tokens",
    )(remote(ids), remote(route), remote(tokens))


def route_tables(got_ref, rows):
    planes, height, _ = got_ref.shape
    span = LANES // rows
    parts = []
    for start in range(0, planes, span):
        total = None
        for plane in range(start, start + span):
            part = got_ref[plane, pl.ds(height - 2 * X, 2 * X), :].astype(F32)
            if plane > start:
                part = pltpu.roll(part, (plane - start) * rows, 1)
            total = part if total is None else total + part
        parts.append(total)
    table = jnp.concatenate(parts, axis=1)
    tokens = planes * rows
    left, right = iota((tokens, tokens), 0), iota((tokens, tokens), 1)
    before = ((left // rows == right // rows) & (left < right)).astype(F32).astype(BF)
    rank = dot_nn((table > 0.0).astype(F32).astype(BF), before)
    return table, rank


def taken_rows(table, rank, j, rows):
    tokens = table.shape[1]
    count = tokens // rows * SLOTS
    row, token = iota((count, tokens), 0), iota((count, tokens), 1)
    return (
        (table[j : j + 1, :] > 0.0)
        & (row // SLOTS == token // rows)
        & (rank[j : j + 1, :] == (row % SLOTS).astype(F32))
    )


def pick_kernel(got_ref, out_ref, tok_ref, pick_ref):
    planes, height, _ = got_ref.shape
    groups = tok_ref.shape[1] // LANES
    rows = (height - 2 * X) // groups
    table, rank = route_tables(got_ref, rows)
    for plane in range(planes):
        for group in range(groups):
            tok_ref[pl.ds(plane * rows, rows), group * LANES : (group + 1) * LANES] = got_ref[
                plane, pl.ds(group * rows, rows), :
            ]
    count = planes * SLOTS
    for j in range(X):
        pick_ref[pl.ds(j * count, count), :] = (
            taken_rows(table, rank, j, rows).astype(F32).astype(BF)
        )
    out_ref[...] = dot_nn(pick_ref[...], tok_ref[...]).astype(BF).reshape(out_ref.shape)


def weigh_kernel(got_ref, high_ref, low_ref):
    planes = got_ref.shape[0]
    rows = high_ref.shape[0] // planes
    table, rank = route_tables(got_ref, rows)
    count = planes * SLOTS
    for j in range(X):
        taken = taken_rows(table, rank, j, rows)
        for ref, line in ((high_ref, j), (low_ref, X + j)):
            value = jnp.where(taken, table[line : line + 1, :], 0.0)
            ref[:, j * count : (j + 1) * count] = value.T.astype(BF)


def join_kernel(got_ref, top_ref, low_ref):
    _, rows, width = got_ref.shape
    half = X // 2
    for x in range(X):
        ref = top_ref if x < half else low_ref
        for core in range(CORES):
            ref[pl.ds((x % half) * rows, rows), core * width : (core + 1) * width] = got_ref[
                x * CORES + core
            ]


def near_kernel(order_ref, *refs):
    pieces, (gate_own, gate_other, up_own, up_other, down_own, down_other) = refs[:6], refs[6:12]
    acc_ref, peak_ref, last_ref, down_ref, x_ref, w_ref, sems = refs[12:]
    core = order_ref[4]
    half, width = pieces[0].shape
    unit = gate_own.shape[0]
    chips = down_own.shape[0]
    own = pl.multiple_of(core * unit, unit)
    other = pl.multiple_of((1 - core) * unit, unit)
    fetched = []
    for number in range(chips):
        lanes = pl.ds(pl.multiple_of(order_ref[number] * width, width), width)
        target = w_ref.at[number] if number < 3 else last_ref
        group = []
        for place, (source, first) in enumerate(
            (
                (gate_own, own),
                (gate_other, other),
                (up_own, own + CORES * unit),
                (up_other, other + CORES * unit),
            )
        ):
            group.append(
                pltpu.make_async_copy(
                    source.at[:, lanes], target.at[pl.ds(first, unit), :], sems.at[number, place]
                )
            )
        fetched.append(group)
    handed = []
    for chip in range(chips):
        for place, (source, first) in enumerate(((down_own, own), (down_other, other))):
            rows = pl.ds(pl.multiple_of(chip * CORES * unit + first, unit), unit)
            handed.append(
                pltpu.make_async_copy(
                    source.at[chip], down_ref.at[rows, :], sems.at[chips + place, chip]
                )
            )
    for copy in [copy for group in fetched for copy in group] + handed:
        copy.start()
    peak = None
    total = None
    for number in range(3):
        x_ref[number, pl.ds(0, half), :] = pieces[2 * number][...]
        x_ref[number, pl.ds(half, half), :] = pieces[2 * number + 1][...]
        x = x_ref[number]
        for copy in fetched[number]:
            copy.wait()
        value = dot_nt(x, w_ref[number])
        total = value if total is None else total + value
        high = jnp.max(jnp.abs(x).astype(F32), axis=0, keepdims=True)
        peak = high if peak is None else jnp.maximum(peak, high)
    acc_ref[...] = total
    peak_ref[...] = peak
    for copy in fetched[3] + handed:
        copy.wait()


def near_chunks(order, pieces, weights, downs):
    half, width = pieces[0].shape
    chips, unit, _ = downs[0].shape
    wide = 2 * CORES * unit
    return pl.pallas_call(
        near_kernel,
        in_specs=[IN_SMEM] + [IN_VMEM] * 6 + [IN_PLACE] * 6,
        out_specs=[IN_VMEM] * 4,
        out_shape=[
            jax.ShapeDtypeStruct((2 * half, wide), F32),
            jax.ShapeDtypeStruct((1, width), F32),
            jax.ShapeDtypeStruct((wide, width), BF),
            jax.ShapeDtypeStruct((chips * CORES * unit, width), BF),
        ],
        scratch_shapes=[
            pltpu.VMEM((3, 2 * half, width), BF),
            pltpu.VMEM((3, wide, width), BF),
            pltpu.SemaphoreType.DMA((chips + 2, 4)),
        ],
        compiler_params=ROOM,
        cost_estimate=pl.CostEstimate(
            flops=12 * half * width * wide, transcendentals=0, bytes_accessed=12 * width * wide
        ),
        name="near_chunks",
    )(
        order,
        *(local(piece) for piece in pieces),
        *(remote(array) for array in weights),
        *(remote(array) for array in downs),
    )


def far_kernel(top_ref, low_ref, table_ref, acc_ref, peak_in, hid_ref, peak_ref, x_ref):
    half = top_ref.shape[0]
    units = hid_ref.shape[1]
    x_ref[pl.ds(0, half), :] = top_ref[...]
    x_ref[pl.ds(half, half), :] = low_ref[...]
    x = x_ref[...]
    value = acc_ref[...] + dot_nt(x, table_ref[...])
    gate = value[:, :units]
    hid_ref[...] = (gate / (1.0 + jnp.exp(-gate)) * value[:, units:]).astype(BF)
    peak = jnp.maximum(jnp.max(peak_in[...]), jnp.max(jnp.abs(x).astype(F32)))
    peak_ref[...] = jnp.full(peak_ref.shape, peak, F32)


def cut_kernel(order_ref, down_ref, *refs):
    outs, sems = refs[:-1], refs[-1]
    width = outs[0].shape[1]
    run_copies(
        [
            pltpu.make_async_copy(
                down_ref.at[:, pl.ds(pl.multiple_of(order_ref[number] * width, width), width)],
                out_ref,
                sems.at[number],
            )
            for number, out_ref in enumerate(outs)
        ]
    )


def stack_kernel(order_ref, *refs):
    pieces, (out_ref, sems) = refs[:-2], refs[-2:]
    run_copies(
        [
            pltpu.make_async_copy(piece, out_ref.at[order_ref[number]], sems.at[number])
            for number, piece in enumerate(pieces)
        ]
    )


def down_kernel(hid_ref, down_ref, peak_in, out_ref, peak_ref, h_ref):
    chips, _, units = hid_ref.shape
    for chip in range(chips):
        h_ref[:, chip * units : (chip + 1) * units] = hid_ref[chip]
    hidden = h_ref[...]
    value = dot_nn(hidden, down_ref[...]).astype(BF)
    _, rows, width = out_ref.shape
    for x in range(X):
        for core in range(CORES):
            out_ref[x * CORES + core] = value[
                x * rows : (x + 1) * rows, core * width : (core + 1) * width
            ]
    peak = jnp.max(jnp.abs(hidden).astype(F32))
    peak_ref[...] = jnp.where(iota(peak_ref.shape, 1) == 0, peak_in[...], peak)


def combine_kernel(high_ref, low_ref, row_ref, out_ref):
    rows = row_ref[...].reshape(high_ref.shape[1], row_ref.shape[2])
    value = dot_nn(high_ref[...], rows) + dot_nn(low_ref[...], rows)
    out_ref[...] = value.astype(BF).reshape(out_ref.shape)


def total_kernel(part_ref, out_ref):
    total = part_ref[0].astype(F32)
    for plane in range(1, part_ref.shape[0]):
        total = total + part_ref[plane].astype(F32)
    out_ref[...] = total.astype(BF)


def layer(tokens, expert_ids, route_weight, gate_weight, up_weight, down_weight):
    planes = lax.axis_size("z")
    chips = lax.axis_size("chip")
    core = lax.axis_index("core")
    place = lax.axis_index("chip")
    rows, width = tokens.shape
    unit, _ = gate_weight.shape[1:]
    chunk = CORES * width
    units = CORES * unit
    kept = X * planes * SLOTS // CORES
    shaped = jax.ShapeDtypeStruct

    def swap(array, mask):
        return lax.ppermute(array, "chip", [(j, j ^ mask) for j in range(chips)])

    def partner(array):
        return lax.ppermute(array, "core", [(j, 1 - j) for j in range(CORES)])

    lane = jnp.arange(8, dtype=jnp.int32)
    order = jnp.where(
        lane < 2, place ^ lane, jnp.where(lane < 4, place ^ (5 - lane), core)
    ).astype(jnp.int32)

    packed = pack_tokens(expert_ids.T, route_weight.T, tokens, planes)
    plane_rows = lax.all_to_all(packed, "z", split_axis=0, concat_axis=0, tiled=True)

    gate_other = partner(gate_weight[0])
    up_other = partner(up_weight[0])
    cuts = move(cut_kernel, order, (down_weight[0],), [shaped((unit, chunk), BF)] * chips, chips)
    pieces = [cuts[0], swap(cuts[1], 1), swap(cuts[2], 3), swap(cuts[3], 2)]
    sent = call(
        pick_kernel,
        None,
        (local(plane_rows),),
        shaped((X * CORES, kept // X, width), BF),
        (
            pltpu.VMEM((planes * rows, width), BF),
            pltpu.VMEM((X * planes * SLOTS, planes * rows), BF),
        ),
    )
    received = lax.all_to_all(sent, ("x", "core"), split_axis=0, concat_axis=0, tiled=True)
    stacked = move(stack_kernel, order, pieces, shaped((chips, unit, chunk), BF), chips)
    stacked_other = partner(stacked)
    high, low = call(
        weigh_kernel,
        None,
        (local(plane_rows),),
        [shaped((planes * rows, X * planes * SLOTS), BF)] * 2,
    )

    top, bottom = call(join_kernel, None, (local(received),), [shaped((kept // 2, chunk), BF)] * 2)
    cross_top = swap(top, 3)
    beside_low = swap(bottom, 1)
    beside_top = swap(top, 1)
    cross_low = swap(bottom, 3)
    far_low = swap(beside_low, 3)
    far_top = swap(cross_top, 1)
    acc, peak, last, down = near_chunks(
        order,
        (top, bottom, beside_top, beside_low, cross_top, cross_low),
        (gate_weight[0], gate_other, up_weight[0], up_other),
        (stacked, stacked_other),
    )
    hidden, peak = call(
        far_kernel,
        None,
        tuple(local(a) for a in (far_top, far_low, last, acc, peak)),
        [shaped((kept, units), BF), shaped((8, LANES), F32)],
        (pltpu.VMEM((kept, chunk), BF),),
    )
    gathered = lax.all_gather(hidden, "chip", axis=0)
    outputs, peak = call(
        down_kernel,
        None,
        tuple(local(a) for a in (gathered, down, peak)),
        [shaped((X * CORES, kept // X, width), BF), shaped((8, LANES), F32)],
        (pltpu.VMEM((kept, chips * units), BF),),
    )
    returned = lax.all_to_all(outputs, ("x", "core"), split_axis=0, concat_axis=0, tiled=True)
    column = jnp.maximum(peak, partner(peak))[:1, :2].T
    sums = call(
        combine_kernel,
        None,
        tuple(local(a) for a in (high, low, returned)),
        shaped((planes, rows, width), BF),
    )
    sums, column = lax.optimization_barrier((sums, column))
    parts = lax.all_to_all(sums, "z", split_axis=0, concat_axis=0, tiled=True)
    moe_out = call(total_kernel, None, (local(parts),), shaped((rows, width), BF))
    return moe_out, column


def solution(mesh):
    devices = np.asarray(mesh.devices)
    ep, tp = devices.shape
    fine = Mesh(
        devices.reshape(X, ep // X, tp // CORES, CORES), ("x", "z", "chip", "core")
    )
    ep, tp = ("x", "z"), ("chip", "core")
    return jax.shard_map(
        layer,
        mesh=fine,
        in_specs=(
            P(ep, tp),
            P(ep, None),
            P(ep, None),
            P(ep, tp, None),
            P(ep, tp, None),
            P(ep, tp, None),
        ),
        out_specs=(P(ep, tp), P(None, ep)),
        check_vma=False,
    )
```

```python
import jax
import jax.numpy as jnp
import numpy as np
from jax import lax
from jax.experimental import pallas as pl
from jax.experimental.pallas import tpu as pltpu
from jax.sharding import Mesh, PartitionSpec as P


TOP = 8
SLOTS = 8
CORES = 2
X = 4
LANES = 128
BF = jnp.bfloat16
F32 = jnp.float32


IN_VMEM = pl.BlockSpec(memory_space=pltpu.VMEM)
IN_PLACE = pl.BlockSpec(memory_space=pltpu.HBM)
IN_SMEM = pl.BlockSpec(memory_space=pltpu.SMEM)
ROOM = pltpu.CompilerParams(vmem_limit_bytes=24 << 20)


def local(array):
    return pltpu.with_memory_space_constraint(array, pltpu.VMEM)


def remote(array):
    return pltpu.with_memory_space_constraint(array, pltpu.HBM)


def dot_nt(a, b):
    return lax.dot_general(a, b, (((1,), (1,)), ((), ())), preferred_element_type=F32)


def dot_nn(a, b):
    return lax.dot_general(a, b, (((1,), (0,)), ((), ())), preferred_element_type=F32)


def iota(shape, axis):
    return lax.broadcasted_iota(jnp.int32, shape, axis)


def run_copies(copies):
    for copy in copies:
        copy.start()
    for copy in copies:
        copy.wait()


def move(kernel, order, inputs, out_shape, count):
    single = isinstance(out_shape, jax.ShapeDtypeStruct)
    return pl.pallas_call(
        kernel,
        in_specs=[IN_SMEM] + [IN_PLACE] * len(inputs),
        out_specs=IN_PLACE if single else [IN_PLACE] * len(out_shape),
        out_shape=out_shape,
        scratch_shapes=[pltpu.SemaphoreType.DMA((count,))],
        compiler_params=ROOM,
    )(order, *(remote(array) for array in inputs))


def call(kernel, order, inputs, out_shape, scratch=(), cost=None):
    single = isinstance(out_shape, jax.ShapeDtypeStruct)
    specs = ([] if order is None else [IN_SMEM]) + [IN_VMEM] * len(inputs)
    run = pl.pallas_call(
        kernel,
        in_specs=specs,
        out_specs=IN_VMEM if single else [IN_VMEM] * len(out_shape),
        out_shape=out_shape,
        scratch_shapes=list(scratch),
        compiler_params=ROOM,
        cost_estimate=cost,
    )
    return run(*(() if order is None else (order,)), *inputs)


def pack_kernel(ids_hbm, route_hbm, tok_hbm, out_ref, ids_ref, route_ref, tok_ref, sems):
    copies = [
        pltpu.make_async_copy(source, target, sems.at[number])
        for number, (source, target) in enumerate(
            ((ids_hbm, ids_ref), (route_hbm, route_ref), (tok_hbm, tok_ref))
        )
    ]
    run_copies(copies)
    planes, height, _ = out_ref.shape
    rows, width = tok_ref.shape
    for group in range(width // LANES):
        piece = tok_ref[:, group * LANES : (group + 1) * LANES]
        for plane in range(planes):
            out_ref[plane, pl.ds(group * rows, rows), :] = piece
    lines = planes * 2 * X
    line = iota((lines, rows), 0)
    expert = (line % X) * planes + line // (2 * X)
    scale = jnp.zeros((lines, rows), F32)
    for k in range(TOP):
        scale = jnp.where(ids_ref[k : k + 1, :] == expert, route_ref[k : k + 1, :], scale)
    high = scale.astype(BF).astype(F32)
    value = jnp.where((line // X) % 2 == 0, high, scale - high).astype(BF)
    spread = (iota((rows, LANES), 1) == iota((rows, LANES), 0)).astype(F32).astype(BF)
    info = dot_nn(value, spread).reshape(planes, 2 * X, LANES)
    out_ref[:, pl.ds(height - 2 * X, 2 * X), :] = info.astype(BF)


def pack_tokens(ids, route, tokens, planes):
    rows, width = tokens.shape
    height = width // LANES * rows + 2 * X
    return pl.pallas_call(
        pack_kernel,
        in_specs=[IN_PLACE] * 3,
        out_specs=IN_VMEM,
        out_shape=jax.ShapeDtypeStruct((planes, height, LANES), BF),
        scratch_shapes=[
            pltpu.VMEM(ids.shape, ids.dtype),
            pltpu.VMEM(route.shape, route.dtype),
            pltpu.VMEM(tokens.shape, tokens.dtype),
            pltpu.SemaphoreType.DMA((3,)),
        ],
        compiler_params=ROOM,
        name="pack_tokens",
    )(remote(ids), remote(route), remote(tokens))


def route_tables(got_ref, rows):
    planes, height, _ = got_ref.shape
    span = LANES // rows
    parts = []
    for start in range(0, planes, span):
        total = None
        for plane in range(start, start + span):
            part = got_ref[plane, pl.ds(height - 2 * X, 2 * X), :].astype(F32)
            if plane > start:
                part = pltpu.roll(part, (plane - start) * rows, 1)
            total = part if total is None else total + part
        parts.append(total)
    table = jnp.concatenate(parts, axis=1)
    tokens = planes * rows
    left, right = iota((tokens, tokens), 0), iota((tokens, tokens), 1)
    before = ((left // rows == right // rows) & (left < right)).astype(F32).astype(BF)
    rank = dot_nn((table > 0.0).astype(F32).astype(BF), before)
    return table, rank


def taken_rows(table, rank, j, rows):
    tokens = table.shape[1]
    count = tokens // rows * SLOTS
    row, token = iota((count, tokens), 0), iota((count, tokens), 1)
    return (
        (table[j : j + 1, :] > 0.0)
        & (row // SLOTS == token // rows)
        & (rank[j : j + 1, :] == (row % SLOTS).astype(F32))
    )


def pick_kernel(got_ref, out_ref, tok_ref, pick_ref):
    planes, height, _ = got_ref.shape
    groups = tok_ref.shape[1] // LANES
    rows = (height - 2 * X) // groups
    table, rank = route_tables(got_ref, rows)
    for plane in range(planes):
        for group in range(groups):
            tok_ref[pl.ds(plane * rows, rows), group * LANES : (group + 1) * LANES] = got_ref[
                plane, pl.ds(group * rows, rows), :
            ]
    count = planes * SLOTS
    for j in range(X):
        pick_ref[pl.ds(j * count, count), :] = (
            taken_rows(table, rank, j, rows).astype(F32).astype(BF)
        )
    out_ref[...] = dot_nn(pick_ref[...], tok_ref[...]).astype(BF).reshape(out_ref.shape)


def weigh_kernel(got_ref, high_ref, low_ref):
    planes = got_ref.shape[0]
    rows = high_ref.shape[0] // planes
    table, rank = route_tables(got_ref, rows)
    count = planes * SLOTS
    for j in range(X):
        taken = taken_rows(table, rank, j, rows)
        for ref, line in ((high_ref, j), (low_ref, X + j)):
            value = jnp.where(taken, table[line : line + 1, :], 0.0)
            ref[:, j * count : (j + 1) * count] = value.T.astype(BF)


def join_kernel(got_ref, top_ref, low_ref):
    _, rows, width = got_ref.shape
    half = X // 2
    for x in range(X):
        ref = top_ref if x < half else low_ref
        for core in range(CORES):
            ref[pl.ds((x % half) * rows, rows), core * width : (core + 1) * width] = got_ref[
                x * CORES + core
            ]


def near_kernel(order_ref, *refs):
    pieces, (gate_own, gate_other, up_own, up_other) = refs[:6], refs[6:10]
    acc_ref, peak_ref, last_ref, x_ref, w_ref, sems = refs[10:]
    core = order_ref[4]
    half, width = pieces[0].shape
    unit = gate_own.shape[0]
    chips = gate_own.shape[1] // width
    own = pl.multiple_of(core * unit, unit)
    other = pl.multiple_of((1 - core) * unit, unit)
    fetched = []
    for number in range(chips):
        lanes = pl.ds(pl.multiple_of(order_ref[number] * width, width), width)
        target = w_ref.at[number] if number < 3 else last_ref
        group = []
        for place, (source, first) in enumerate(
            (
                (gate_own, own),
                (gate_other, other),
                (up_own, own + CORES * unit),
                (up_other, other + CORES * unit),
            )
        ):
            group.append(
                pltpu.make_async_copy(
                    source.at[:, lanes], target.at[pl.ds(first, unit), :], sems.at[number, place]
                )
            )
        fetched.append(group)
    for copy in [copy for group in fetched for copy in group]:
        copy.start()
    peak = None
    total = None
    for number in range(3):
        x_ref[number, pl.ds(0, half), :] = pieces[2 * number][...]
        x_ref[number, pl.ds(half, half), :] = pieces[2 * number + 1][...]
        x = x_ref[number]
        for copy in fetched[number]:
            copy.wait()
        value = dot_nt(x, w_ref[number])
        total = value if total is None else total + value
        high = jnp.max(jnp.abs(x).astype(F32), axis=0, keepdims=True)
        peak = high if peak is None else jnp.maximum(peak, high)
    acc_ref[...] = total
    peak_ref[...] = peak
    for copy in fetched[3]:
        copy.wait()


def near_chunks(order, pieces, weights):
    half, width = pieces[0].shape
    unit, every = weights[0].shape
    chips = every // width
    wide = 2 * CORES * unit
    return pl.pallas_call(
        near_kernel,
        in_specs=[IN_SMEM] + [IN_VMEM] * 6 + [IN_PLACE] * 4,
        out_specs=[IN_VMEM] * 3,
        out_shape=[
            jax.ShapeDtypeStruct((2 * half, wide), F32),
            jax.ShapeDtypeStruct((1, width), F32),
            jax.ShapeDtypeStruct((wide, width), BF),
        ],
        scratch_shapes=[
            pltpu.VMEM((3, 2 * half, width), BF),
            pltpu.VMEM((3, wide, width), BF),
            pltpu.SemaphoreType.DMA((chips, 4)),
        ],
        compiler_params=ROOM,
        cost_estimate=pl.CostEstimate(
            flops=12 * half * width * wide, transcendentals=0, bytes_accessed=12 * width * wide
        ),
        name="near_chunks",
    )(
        order,
        *(local(piece) for piece in pieces),
        *(remote(array) for array in weights),
    )


def far_kernel(top_ref, low_ref, table_ref, acc_ref, peak_in, hid_ref, peak_ref, x_ref):
    half = top_ref.shape[0]
    units = hid_ref.shape[1]
    x_ref[pl.ds(0, half), :] = top_ref[...]
    x_ref[pl.ds(half, half), :] = low_ref[...]
    x = x_ref[...]
    value = acc_ref[...] + dot_nt(x, table_ref[...])
    gate = value[:, :units]
    hid_ref[...] = (gate / (1.0 + jnp.exp(-gate)) * value[:, units:]).astype(BF)
    peak = jnp.maximum(jnp.max(peak_in[...]), jnp.max(jnp.abs(x).astype(F32)))
    peak_ref[...] = jnp.full(peak_ref.shape, peak, F32)


def cut_kernel(order_ref, down_ref, *refs):
    outs, sems = refs[:-1], refs[-1]
    width = outs[0].shape[1]
    run_copies(
        [
            pltpu.make_async_copy(
                down_ref.at[:, pl.ds(pl.multiple_of(order_ref[number] * width, width), width)],
                out_ref,
                sems.at[number],
            )
            for number, out_ref in enumerate(outs)
        ]
    )


def stack_kernel(order_ref, *refs):
    pieces, (out_ref, sems) = refs[:-2], refs[-2:]
    run_copies(
        [
            pltpu.make_async_copy(piece, out_ref.at[order_ref[number]], sems.at[number])
            for number, piece in enumerate(pieces)
        ]
    )


def pair_kernel(order_ref, own_ref, other_ref, out_ref, sems):
    chips, unit, _ = own_ref.shape
    core = order_ref[4]
    copies = []
    for chip in range(chips):
        for number, (source, place) in enumerate(((own_ref, core), (other_ref, 1 - core))):
            first = pl.multiple_of((chip * CORES + place) * unit, unit)
            copies.append(
                pltpu.make_async_copy(
                    source.at[chip], out_ref.at[pl.ds(first, unit), :], sems.at[chip, number]
                )
            )
    run_copies(copies)


def pair_rows(order, own, other):
    chips, unit, width = own.shape
    return pl.pallas_call(
        pair_kernel,
        in_specs=[IN_SMEM] + [IN_PLACE] * 2,
        out_specs=IN_VMEM,
        out_shape=jax.ShapeDtypeStruct((chips * CORES * unit, width), BF),
        scratch_shapes=[pltpu.SemaphoreType.DMA((chips, CORES))],
        compiler_params=ROOM,
        name="pair_rows",
    )(order, remote(own), remote(other))


def down_kernel(hid_ref, down_ref, peak_in, out_ref, peak_ref, h_ref):
    chips, _, units = hid_ref.shape
    for chip in range(chips):
        h_ref[:, chip * units : (chip + 1) * units] = hid_ref[chip]
    hidden = h_ref[...]
    value = dot_nn(hidden, down_ref[...]).astype(BF)
    _, rows, width = out_ref.shape
    for x in range(X):
        for core in range(CORES):
            out_ref[x * CORES + core] = value[
                x * rows : (x + 1) * rows, core * width : (core + 1) * width
            ]
    peak = jnp.max(jnp.abs(hidden).astype(F32))
    peak_ref[...] = jnp.where(iota(peak_ref.shape, 1) == 0, peak_in[...], peak)


def combine_kernel(high_ref, low_ref, row_ref, out_ref):
    rows = row_ref[...].reshape(high_ref.shape[1], row_ref.shape[2])
    value = dot_nn(high_ref[...], rows) + dot_nn(low_ref[...], rows)
    out_ref[...] = value.astype(BF).reshape(out_ref.shape)


def total_kernel(part_ref, out_ref):
    total = part_ref[0].astype(F32)
    for plane in range(1, part_ref.shape[0]):
        total = total + part_ref[plane].astype(F32)
    out_ref[...] = total.astype(BF)


def layer(tokens, expert_ids, route_weight, gate_weight, up_weight, down_weight):
    planes = lax.axis_size("z")
    chips = lax.axis_size("chip")
    core = lax.axis_index("core")
    place = lax.axis_index("chip")
    rows, width = tokens.shape
    unit, _ = gate_weight.shape[1:]
    chunk = CORES * width
    units = CORES * unit
    kept = X * planes * SLOTS // CORES
    shaped = jax.ShapeDtypeStruct

    def swap(array, mask):
        return lax.ppermute(array, "chip", [(j, j ^ mask) for j in range(chips)])

    def partner(array):
        return lax.ppermute(array, "core", [(j, 1 - j) for j in range(CORES)])

    lane = jnp.arange(8, dtype=jnp.int32)
    order = jnp.where(
        lane < 2, place ^ lane, jnp.where(lane < 4, place ^ (5 - lane), core)
    ).astype(jnp.int32)

    packed = pack_tokens(expert_ids.T, route_weight.T, tokens, planes)
    plane_rows = lax.all_to_all(packed, "z", split_axis=0, concat_axis=0, tiled=True)

    gate_other = partner(gate_weight[0])
    up_other = partner(up_weight[0])
    cuts = move(cut_kernel, order, (down_weight[0],), [shaped((unit, chunk), BF)] * chips, chips)
    pieces = [cuts[0], swap(cuts[1], 1), swap(cuts[2], 3), swap(cuts[3], 2)]
    sent = call(
        pick_kernel,
        None,
        (local(plane_rows),),
        shaped((X * CORES, kept // X, width), BF),
        (
            pltpu.VMEM((planes * rows, width), BF),
            pltpu.VMEM((X * planes * SLOTS, planes * rows), BF),
        ),
    )
    received = lax.all_to_all(sent, ("x", "core"), split_axis=0, concat_axis=0, tiled=True)
    stacked = move(stack_kernel, order, pieces, shaped((chips, unit, chunk), BF), chips)
    stacked_other = partner(stacked)
    down = pair_rows(order, stacked, stacked_other)
    high, low = call(
        weigh_kernel,
        None,
        (local(plane_rows),),
        [shaped((planes * rows, X * planes * SLOTS), BF)] * 2,
    )

    top, bottom = call(join_kernel, None, (local(received),), [shaped((kept // 2, chunk), BF)] * 2)
    cross_top = swap(top, 3)
    beside_low = swap(bottom, 1)
    cross_low = swap(bottom, 3)
    beside_top = swap(top, 1)
    far_top, far_low = swap(cross_top, 1), swap(beside_low, 3)
    acc, peak, last = near_chunks(
        order,
        (top, bottom, beside_top, beside_low, cross_top, cross_low),
        (gate_weight[0], gate_other, up_weight[0], up_other),
    )
    hidden, peak = call(
        far_kernel,
        None,
        tuple(local(a) for a in (far_top, far_low, last, acc, peak)),
        [shaped((kept, units), BF), shaped((8, LANES), F32)],
        (pltpu.VMEM((kept, chunk), BF),),
    )
    gathered = lax.all_gather(hidden, "chip", axis=0)
    outputs, peak = call(
        down_kernel,
        None,
        tuple(local(a) for a in (gathered, down, peak)),
        [shaped((X * CORES, kept // X, width), BF), shaped((8, LANES), F32)],
        (pltpu.VMEM((kept, chips * units), BF),),
    )
    returned = lax.all_to_all(outputs, ("x", "core"), split_axis=0, concat_axis=0, tiled=True)
    column = jnp.maximum(peak, partner(peak))[:1, :2].T
    sums = call(
        combine_kernel,
        None,
        tuple(local(a) for a in (high, low, returned)),
        shaped((planes, rows, width), BF),
    )
    sums, column = lax.optimization_barrier((sums, column))
    parts = lax.all_to_all(sums, "z", split_axis=0, concat_axis=0, tiled=True)
    moe_out = call(total_kernel, None, (local(parts),), shaped((rows, width), BF))
    return moe_out, column


def solution(mesh):
    devices = np.asarray(mesh.devices)
    ep, tp = devices.shape
    fine = Mesh(
        devices.reshape(X, ep // X, tp // CORES, CORES), ("x", "z", "chip", "core")
    )
    ep, tp = ("x", "z"), ("chip", "core")
    return jax.shard_map(
        layer,
        mesh=fine,
        in_specs=(
            P(ep, tp),
            P(ep, None),
            P(ep, None),
            P(ep, tp, None),
            P(ep, tp, None),
            P(ep, tp, None),
        ),
        out_specs=(P(ep, tp), P(None, ep)),
        check_vma=False,
    )
```
